32 devices in a mesh: rep: 2 (over z, core), dp: 16 (over x, y).
Axes of the slice: x: 4, y: 4, z: 1, core: 2. Of those that a mesh axis runs over, the one named last changes fastest.
The devices are a block of a 4x4x8 slice.
Arguments:
- g_w_gate: bfloat16 [32, 2, 512, 4096], P(('rep', 'dp')), parts along dimension 0
- g_w_up: bfloat16 [32, 2, 512, 4096], P(('rep', 'dp')), parts along dimension 0
- g_w_down: bfloat16 [32, 2, 4096, 512], P(('rep', 'dp')), parts along dimension 0
- w_gate: bfloat16 [2, 512, 4096], replicated
- w_up: bfloat16 [2, 512, 4096], replicated
- w_down: bfloat16 [2, 4096, 512], replicated
- m_w_gate: float32 [2, 512, 4096], P(None, 'dp')
- m_w_up: float32 [2, 512, 4096], P(None, 'dp')
- m_w_down: float32 [2, 4096, 512], P(None, 'dp')
- v_w_gate: float32 [2, 512, 4096], P(None, 'dp')
- v_w_up: float32 [2, 512, 4096], P(None, 'dp')
- v_w_down: float32 [2, 4096, 512], P(None, 'dp')
Outputs:
- output 1: bfloat16 [4, 512, 4096], P('rep'), parts along dimension 0
- output 2: bfloat16 [4, 512, 4096], P('rep'), parts along dimension 0
- output 3: bfloat16 [4, 4096, 512], P('rep'), parts along dimension 0
- output 4: float32 [4, 512, 4096], P('rep', 'dp'), parts along dimension 0
- output 5: float32 [4, 512, 4096], P('rep', 'dp'), parts along dimension 0
- output 6: float32 [4, 4096, 512], P('rep', 'dp'), parts along dimension 0
- output 7: float32 [4, 512, 4096], P('rep', 'dp'), parts along dimension 0
- output 8: float32 [4, 512, 4096], P('rep', 'dp'), parts along dimension 0
- output 9: float32 [4, 4096, 512], P('rep', 'dp'), parts along dimension 0
There are 2 independent parts. The reference program is written for one: setup_inputs(seed, part) draws one part's arguments, and reference() takes and returns one part's arrays. A program takes and returns all parts, laid end to end along the dimension named above; an argument that names none is the same for every part.
All inputs are finite; a program needn't handle non-finite values.
Results may differ from the reference program's by a relative error of at most 0.022.
Values are sent between devices in bfloat16 or wider.
A program may use at most 768 MiB of HBM per device.

```python
import jax
import jax.numpy as jnp
from jax import lax

DEVICES = 16
D = 512
FF = 4096
LAYERS = 2
NAMES = ("w_gate", "w_up", "w_down")
SHAPES = {"w_gate": (LAYERS, D, FF), "w_up": (LAYERS, D, FF), "w_down": (LAYERS, FF, D)}


def setup_inputs(seed: int = 0, part: int = 0) -> dict:
    kz, *keys = jax.random.split(jax.random.key(seed), 1 + 5 * len(NAMES))
    loud = 2.0 ** jax.random.uniform(kz, (), jnp.float32, -1.0, 1.0)
    drawn = {}
    for name, key, both in zip(NAMES, keys[:3], keys[3:6], strict=True):
        own = jax.random.normal(jax.random.fold_in(key, part), (DEVICES, *SHAPES[name]), jnp.float32)
        shared = jax.random.normal(jax.random.fold_in(both, part), SHAPES[name], jnp.float32)
        drawn["g_" + name] = (loud * (0.7 * shared / DEVICES + 0.7 * own * DEVICES**-0.5)).astype(jnp.bfloat16)
    for name, key in zip(NAMES, keys[6:9], strict=True):
        drawn[name] = (jax.random.normal(key, SHAPES[name], jnp.float32) * SHAPES[name][1] ** -0.5).astype(jnp.bfloat16)
    for name, key in zip(NAMES, keys[9:12], strict=True):
        drawn["m_" + name] = loud * 0.5 * jax.random.normal(key, SHAPES[name], jnp.float32)
    for name, key in zip(NAMES, keys[12:15], strict=True):
        drawn["v_" + name] = loud * loud * jax.random.uniform(key, SHAPES[name], jnp.float32, 0.5, 1.5)
    return drawn


def adamw(w, m, v, g):
    m = 0.9 * m + 0.1 * g
    v = 0.95 * v + 0.05 * g * g
    step = m * lax.rsqrt(v + 1e-8) + 0.1 * w
    return (w - 0.02 * step).astype(jnp.bfloat16), m, v


def clipped(gradients, sum_of_squares, count):
    factor = jnp.minimum(1.0, 0.5 * lax.rsqrt(sum_of_squares / count + 1e-30))
    return [g * factor for g in gradients]


def reference(g_w_gate, g_w_up, g_w_down, w_gate, w_up, w_down, m_w_gate, m_w_up, m_w_down, v_w_gate, v_w_up, v_w_down):
    def total(terms):
        return lax.scan(lambda so_far, term: (so_far + term.astype(jnp.float32), None), jnp.zeros(terms.shape[1:], jnp.float32), terms)[0]

    gradients = [total(terms).astype(jnp.bfloat16).astype(jnp.float32) for terms in (g_w_gate, g_w_up, g_w_down)]
    gradients = clipped(gradients, sum(jnp.sum(g * g) for g in gradients), sum(g.size for g in gradients))
    new = [
        adamw(w.astype(jnp.float32), m, v, g)
        for w, m, v, g in zip((w_gate, w_up, w_down), (m_w_gate, m_w_up, m_w_down), (v_w_gate, v_w_up, v_w_down), gradients, strict=True)
    ]
    return tuple(one[which] for which in range(3) for one in new)
```

```python
import functools
import math

import jax
import jax.numpy as jnp
from jax import lax
from jax.experimental import pallas as pl
from jax.experimental.pallas import tpu as pltpu
from jax.sharding import PartitionSpec as P

MESH = pl.DeviceIdType.MESH
ROWS, COLUMNS = 16, 512
BF16, F32 = jnp.bfloat16, jnp.float32


def tiles(rows, columns, body):
    across = columns // COLUMNS

    def one(t, carry):
        r, c = t // across, t % across
        return body(pl.ds(pl.multiple_of(r * ROWS, ROWS), ROWS), pl.ds(pl.multiple_of(c * COLUMNS, COLUMNS), COLUMNS), carry)

    return functools.partial(lax.fori_loop, 0, (rows // ROWS) * across, one)


def kernel(n, count, *refs):
    side = math.isqrt(n)
    g, w, m, v, whole, new_m, new_v = (refs[3 * i : 3 * i + 3] for i in range(7))
    opp1, fin1, opp2, fin2, own_w = (refs[21 + 3 * i : 24 + 3 * i] for i in range(5))
    squares, mine, load_sem, state_sem, send1, recv1, send2, recv2, send_sq, recv_sq = refs[36:]

    me = lax.axis_index("dp")
    x, y = me // side, me % side
    layers, which = (0, 1), (0, 1, 2)
    size = [(r.shape[-2], r.shape[-1]) for r in new_m]
    low = [pl.ds(0, r // 2) for r, _ in size]
    high = [pl.ds(r // 2, r // 2) for r, _ in size]
    everything = [pl.ds(0, r) for r, _ in size]

    def ab(l):
        return (x, y) if l == 0 else (y, x)

    def at(l, a, b):
        a, b = lax.rem(a, side), lax.rem(b, side)
        return (l, a, b) if l == 0 else (l, b, a)

    def device(l, a, b):
        _, p, q = at(l, a, b)
        return {"dp": p * side + q}

    def remote(src, dst, send, recv, target):
        return pltpu.make_async_remote_copy(src_ref=src, dst_ref=dst, send_sem=send, recv_sem=recv, device_id=target, device_id_type=MESH)

    def sum1(k, l, i, j):
        a, b = ab(l)
        step, rows = ((1, low), (3, high), (1, high), (3, low), (1, low), (3, high))[k]
        rows = rows[i]
        block = at(l, a + 2 if k < 2 else a + step, b + j)
        src = (g if k < 4 else whole)[i].at[(*block, rows)]
        way = k % 2
        dst = opp1[i].at[l, way, j] if k < 2 else fin1[i].at[l, way, j, rows]
        return remote(src, dst, send1.at[i, l, j, k], recv1.at[i, l, j, k], device(l, a + step, b))

    def sum2(k, l, i):
        a, b = ab(l)
        step, rows = ((1, low), (3, high), (1, high), (3, low), (1, low), (3, high))[k]
        rows = rows[i]
        src = whole[i].at[(*at(l, a, b + 2 if k < 2 else b + step), rows)]
        way = k % 2
        dst = opp2[i].at[l, way] if k < 2 else fin2[i].at[l, way, rows]
        return remote(src, dst, send2.at[i, l, k], recv2.at[i, l, k], device(l, a, b + step))

    def gather2(k, l, i):
        a, b = ab(l)
        step, rows, off = ((1, low, 0), (3, high, 0), (1, high, 0), (3, low, 0), (1, low, 3), (3, high, 1))[k]
        block = whole[i].at[(*at(l, a, b + off), rows[i])]
        return remote(block, block, send2.at[i, l, k], recv2.at[i, l, k], device(l, a, b + step))

    def gather1(k, l, i, j):
        a, b = ab(l)
        step, rows, off = ((1, low, 0), (3, high, 0), (1, high, 0), (3, low, 0), (1, low, 3), (3, high, 1))[k]
        block = whole[i].at[(*at(l, a + off, b + j), rows[i])]
        return remote(block, block, send1.at[i, l, j, k], recv1.at[i, l, j, k], device(l, a + step, b))

    def add(i, rows, block, *terms):
        start, height = rows.start, rows.size

        def body(r, c, carry):
            r = pl.ds(pl.multiple_of(r.start + start, ROWS), ROWS)
            total = whole[i][(*block, r, c)].astype(F32)
            for ref, lead, first in terms:
                total = total + ref[(*lead, pl.ds(pl.multiple_of(r.start - first, ROWS), ROWS), c)].astype(F32)
            whole[i][(*block, r, c)] = total.astype(BF16)
            return carry

        tiles(height, size[i][1], body)(0)

    def load(l, i, s):
        a, _ = ab(l)
        slab = lax.rem(a + (1, 3, 0)[s], side)
        where = (l, slab) if l == 0 else (l, slice(None), slab)
        return pltpu.make_async_copy(g[i].at[where], whole[i].at[where], load_sem.at[i, l, s])

    def states(i):
        return (
            pltpu.make_async_copy(m[i], new_m[i], state_sem.at[i, 0]),
            pltpu.make_async_copy(v[i], new_v[i], state_sem.at[i, 1]),
            *(pltpu.make_async_copy(w[i].at[l, x, y], own_w[i].at[l], state_sem.at[i, 2 + l]) for l in layers),
        )

    for i in which:
        for l in layers:
            for s in (0, 1):
                load(l, i, s).start()

    barrier = pltpu.get_barrier_semaphore()

    def greet(k, carry):
        pl.semaphore_signal(barrier, inc=1, device_id={"dp": lax.rem(me + k, n)}, device_id_type=MESH)
        return carry

    lax.fori_loop(1, n, greet, 0)
    pl.semaphore_wait(barrier, n - 1)

    def send_raw(i, j):
        for k in (0, 1, 2, 3):
            for l in layers:
                sum1(k, l, i, j).start()

    def pass_on1(i, j, first):
        for l in layers:
            a, b = ab(l)
            for k in (0, 1):
                if first:
                    load(l, i, k).wait()
                sum1(k, l, i, j).wait_recv()
                rows = (low, high)[k][i]
                add(i, rows, at(l, a + (1, 3)[k], b + j), (opp1[i], (l, k, j), rows.start))
                sum1(4 + k, l, i, j).start()

    def arrived1(l, i, j, rows):
        for k in (4, 3) if rows == "low" else (2, 5):
            sum1(k, l, i, j).wait_recv()

    def start2(i):
        for l in layers:
            a, b = ab(l)
            load(l, i, 2).wait()
            arrived1(l, i, 2, "low")
            arrived1(l, i, 2, "high")
            add(i, everything[i], at(l, a, b + 2), (fin1[i], (l, 0, 2), 0), (fin1[i], (l, 1, 2), 0))
            sum2(0, l, i).start()
            sum2(1, l, i).start()
        for l in layers:
            a, b = ab(l)
            for k, j, rows, name in ((2, 1, high, "high"), (3, 3, low, "low")):
                arrived1(l, i, j, name)
                add(i, rows[i], at(l, a, b + j), (fin1[i], (l, 0, j), 0), (fin1[i], (l, 1, j), 0))
                sum2(k, l, i).start()

    def pass_on2(i):
        for l in layers:
            a, b = ab(l)
            for k, j, rows, name in ((0, 1, low, "low"), (1, 3, high, "high")):
                arrived1(l, i, j, name)
                sum2(k, l, i).wait_recv()
                add(i, rows[i], at(l, a, b + j), (fin1[i], (l, 0, j), 0), (fin1[i], (l, 1, j), 0), (opp2[i], (l, k), rows[i].start))
                sum2(4 + k, l, i).start()

    def own(i, total):
        for l in layers:
            a, b = ab(l)
            arrived1(l, i, 0, "low")
            arrived1(l, i, 0, "high")
            for k in (2, 3, 4, 5):
                sum2(k, l, i).wait_recv()

            def body(r, c, total, l=l):
                s = whole[i][l, x, y, r, c].astype(F32)
                for ref, lead in ((fin1[i], (l, 0, 0)), (fin1[i], (l, 1, 0)), (fin2[i], (l, 0)), (fin2[i], (l, 1))):
                    s = s + ref[(*lead, r, c)].astype(F32)
                s = s.astype(BF16)
                whole[i][l, x, y, r, c] = s
                s = s.astype(F32)
                return total + s * s

            total = tiles(*size[i], body)(total)
        return total

    def order(t):
        return (3 - t) * (4 - t) // 2 % side

    send_raw(0, 2)

    for i in which:
        for l in layers:
            load(l, i, 2).start()
        for one in states(i):
            one.start()

    def sums(t, first):
        for i in which:
            send_raw((i + 1) % 3, order(t) if i < 2 else order(t + 1))
            pass_on1(i, order(t), first)

    sums(0, True)

    def more(t, carry):
        sums(t, False)
        return carry

    lax.fori_loop(1, side - 1, more, 0)
    for i in which:
        if i < 2:
            send_raw(i + 1, 0)
        start2(i)
        if i > 0:
            pass_on2(i - 1)
        pass_on1(i, 0, False)
    pass_on2(2)

    total = jnp.zeros((ROWS, COLUMNS), F32)
    for i in which:
        total = own(i, total)
    total = jnp.sum(total.reshape(ROWS // 8, 8, COLUMNS), 0)
    mine[...] = functools.reduce(jnp.add, [total[:, 128 * q : 128 * (q + 1)] for q in range(COLUMNS // 128)])

    def sent(t, carry):
        l, k = t // 6, t % 6
        for i in which:
            half = fin2[i].at[0, 0, low[i]]
            for j in range(side):
                pltpu.make_async_copy(half, half, send1.at[i, l, j, k]).wait()
            pltpu.make_async_copy(half, half, send2.at[i, l, k]).wait()
        return carry

    lax.fori_loop(0, 12, sent, 0)

    def share(k):
        return remote(mine, squares.at[me], send_sq.at[k], recv_sq.at[me], {"dp": lax.rem(me + k, n)})

    def told(k):
        other = lax.rem(me + k, n)
        return remote(mine, squares.at[other], send_sq.at[k], recv_sq.at[other], {"dp": other})

    lax.fori_loop(1, n, lambda k, c: (share(k).start(), c)[1], 0)
    squares[me] = mine[...]
    for i in which:
        for one in states(i):
            one.wait()
    lax.fori_loop(1, n, lambda k, c: (told(k).wait_recv(), c)[1], 0)
    total = functools.reduce(jnp.add, [squares[k] for k in range(n)])
    total = jnp.full((8, 128), jnp.sum(total), F32)
    factor = jnp.max(jnp.minimum(1.0, 0.5 * lax.rsqrt(total / count + 1e-30)))

    def update(l, i):
        def body(r, c, carry):
            grad = whole[i][l, x, y, r, c].astype(F32) * factor
            old = own_w[i][l, r, c].astype(F32)
            moment = 0.9 * new_m[i][l, r, c] + 0.1 * grad
            square = 0.95 * new_v[i][l, r, c] + 0.05 * grad * grad
            step = moment * lax.rsqrt(square + 1e-8) + 0.1 * old
            whole[i][l, x, y, r, c] = (old - 0.02 * step).astype(BF16)
            new_m[i][l, r, c] = moment
            new_v[i][l, r, c] = square
            return carry

        tiles(*size[i], body)(0)

    def first(i, j):
        for k in (0, 1, 2, 3):
            for l in layers:
                gather1(k, l, i, j).start()

    def forward1(i, j):
        for k in (0, 1):
            for l in layers:
                gather1(k, l, i, j).wait_recv()
                gather1(4 + k, l, i, j).start()

    def forward2(i):
        for k in (0, 1):
            for l in layers:
                gather2(k, l, i).wait_recv()
                gather2(4 + k, l, i).start()

    for i in which:
        for l in layers:
            update(l, i)
            for k in (0, 1, 2, 3):
                gather2(k, l, i).start()
        if i == 0:
            first(0, 0)
    forward2(0)
    first(1, 0)
    forward2(1)
    first(2, 0)
    forward1(0, 0)
    forward2(2)
    forward1(1, 0)

    def back(t):
        return t * (t + 1) // 2 % side

    def gathers(t, i):
        first(i, back(t))
        forward1((i + 2) % 3, back(t) if i > 0 else back(t - 1))

    for i in which:
        for k in (2, 3, 4, 5):
            for l in layers:
                gather2(k, l, i).wait_recv()
        gathers(1, i)

    def rest(t, carry):
        for i in which:
            gathers(t, i)
        return carry

    lax.fori_loop(2, side, rest, 0)
    forward1(2, 2)

    def landed(t, carry):
        l, k = t // 4, 2 + t % 4
        for i in which:
            half = fin2[i].at[0, 0, low[i]]
            for j in range(side):
                pltpu.make_async_copy(half, half, recv1.at[i, l, j, k]).wait()
        return carry

    lax.fori_loop(0, 8, landed, 0)
    lax.fori_loop(0, 12, sent, 0)
    lax.fori_loop(1, n, lambda k, c: (share(k).wait_send(), c)[1], 0)


def drain(*refs):
    sources, targets, sem = refs[:9], refs[9:18], refs[18]
    copies = [pltpu.make_async_copy(s, t, sem.at[k]) for k, (s, t) in enumerate(zip(sources, targets, strict=True))]
    for copy in copies:
        copy.start()
    for copy in copies:
        copy.wait()


def solution(mesh):
    n = mesh.shape["dp"]
    side = math.isqrt(n)

    def step(*arrays):
        terms, weights, m, v = (arrays[i : i + 3] for i in (0, 3, 6, 9))
        count = n * sum(one.size for one in m)
        blocks = [one.shape for one in m]
        grid = [(l, side, side, r, c) for l, r, c in blocks]
        any_of = pl.BlockSpec(memory_space=pl.ANY)
        half = lambda *lead: [pltpu.VMEM((*lead, r // 2, c), BF16) for _, r, c in blocks]
        full = lambda *lead: [pltpu.VMEM((*lead, r, c), BF16) for _, r, c in blocks]
        dma = pltpu.SemaphoreType.DMA
        out = pl.pallas_call(
            functools.partial(kernel, n, count),
            out_shape=[pltpu.VMEM(one, BF16) for one in grid] + [pltpu.VMEM(one, F32) for one in blocks] * 2,
            in_specs=[any_of] * 12,
            out_specs=[pl.BlockSpec(memory_space=pltpu.VMEM)] * 9,
            scratch_shapes=[
                *half(2, 2, side),
                *full(2, 2, side),
                *half(2, 2),
                *full(2, 2),
                *full(2),
                pltpu.VMEM((n, 8, 128), F32),
                pltpu.VMEM((8, 128), F32),
                dma((3, 2, 3)),
                dma((3, 4)),
                dma((3, 2, side, 6)),
                dma((3, 2, side, 6)),
                dma((3, 2, 6)),
                dma((3, 2, 6)),
                dma((n,)),
                dma((n,)),
            ],
            compiler_params=pltpu.CompilerParams(collective_id=0, has_side_effects=True, vmem_limit_bytes=25 << 20),
            name="step",
        )(
            *(t.reshape(one) for t, one in zip(terms, grid, strict=True)),
            *(t.reshape(one) for t, one in zip(weights, grid, strict=True)),
            *m,
            *v,
        )
        out = pl.pallas_call(
            drain,
            out_shape=[jax.ShapeDtypeStruct(one, BF16) for one in grid] + [jax.ShapeDtypeStruct(one, F32) for one in blocks] * 2,
            in_specs=[any_of] * 9,
            out_specs=[any_of] * 9,
            scratch_shapes=[dma((9,))],
            compiler_params=pltpu.CompilerParams(vmem_limit_bytes=1 << 20),
            name="drain",
        )(*(pltpu.with_memory_space_constraint(one, pltpu.VMEM) for one in out))
        return (*(one.reshape(w.shape) for one, w in zip(out[:3], weights, strict=True)), *out[3:])

    all_of, cut = P(None, None, None), P(None, "dp", None)
    return jax.shard_map(
        step,
        mesh=mesh,
        in_specs=(P(("rep", "dp"), None, None, None),) * 3 + (all_of,) * 3 + (cut,) * 6,
        out_specs=(P("rep", None, None),) * 3 + (P("rep", "dp", None),) * 6,
        check_vma=False,
    )
```

```python
import functools
import math

import jax
import jax.numpy as jnp
from jax import lax
from jax.experimental import pallas as pl
from jax.experimental.pallas import tpu as pltpu
from jax.sharding import PartitionSpec as P

MESH = pl.DeviceIdType.MESH
ROWS, COLUMNS = 16, 512
BF16, F32 = jnp.bfloat16, jnp.float32


def tiles(rows, columns, body):
    across = columns // COLUMNS

    def one(t, carry):
        r, c = t // across, t % across
        return body(pl.ds(pl.multiple_of(r * ROWS, ROWS), ROWS), pl.ds(pl.multiple_of(c * COLUMNS, COLUMNS), COLUMNS), carry)

    return functools.partial(lax.fori_loop, 0, (rows // ROWS) * across, one)


def kernel(n, count, *refs):
    side = math.isqrt(n)
    g, w, m, v, whole, new_m, new_v = (refs[3 * i : 3 * i + 3] for i in range(7))
    opp1, fin1, opp2, fin2, own_w = (refs[21 + 3 * i : 24 + 3 * i] for i in range(5))
    squares, mine, load_sem, state_sem, send1, send2, early1, late1, early2, late2, send_sq, recv_sq = refs[36:]

    me = lax.axis_index("dp")
    x, y = me // side, me % side
    layers, which = (0, 1), (0, 1, 2)
    size = [(r.shape[-2], r.shape[-1]) for r in new_m]
    low = [pl.ds(0, r // 2) for r, _ in size]
    high = [pl.ds(r // 2, r // 2) for r, _ in size]
    everything = [pl.ds(0, r) for r, _ in size]

    def ab(l):
        return (x, y) if l == 0 else (y, x)

    def at(l, a, b):
        a, b = lax.rem(a, side), lax.rem(b, side)
        return (l, a, b) if l == 0 else (l, b, a)

    def device(l, a, b):
        _, p, q = at(l, a, b)
        return {"dp": p * side + q}

    def remote(src, dst, send, recv, target):
        return pltpu.make_async_remote_copy(src_ref=src, dst_ref=dst, send_sem=send, recv_sem=recv, device_id=target, device_id_type=MESH)

    def sum1(k, l, i, j):
        a, b = ab(l)
        step, rows = ((1, low), (3, high), (1, high), (3, low), (1, low), (3, high))[k]
        rows = rows[i]
        block = at(l, a + 2 if k < 2 else a + step, b + j)
        src = (g if k < 4 else whole)[i].at[(*block, rows)]
        way = k % 2
        dst = opp1[i].at[l, way, j] if k < 2 else fin1[i].at[l, way, j, rows]
        return remote(src, dst, send1.at[i], (early1 if k < 2 else late1).at[i, j], device(l, a + step, b))

    def sum2(k, l, i):
        a, b = ab(l)
        step, rows = ((1, low), (3, high), (1, high), (3, low), (1, low), (3, high))[k]
        rows = rows[i]
        src = whole[i].at[(*at(l, a, b + 2 if k < 2 else b + step), rows)]
        way = k % 2
        dst = opp2[i].at[l, way] if k < 2 else fin2[i].at[l, way, rows]
        return remote(src, dst, send2.at[i], (early2 if k < 2 else late2).at[i], device(l, a, b + step))

    def gather2(k, l, i):
        a, b = ab(l)
        step, rows, off = ((1, low, 0), (3, high, 0), (1, high, 0), (3, low, 0), (1, low, 3), (3, high, 1))[k]
        block = whole[i].at[(*at(l, a, b + off), rows[i])]
        return remote(block, block, send2.at[i], (early2 if k < 2 else late2).at[i], device(l, a, b + step))

    def gather1(k, l, i, j):
        a, b = ab(l)
        step, rows, off = ((1, low, 0), (3, high, 0), (1, high, 0), (3, low, 0), (1, low, 3), (3, high, 1))[k]
        block = whole[i].at[(*at(l, a + off, b + j), rows[i])]
        return remote(block, block, send1.at[i], (early1 if k < 2 else late1).at[i, j], device(l, a + step, b))

    def add(i, rows, block, *terms):
        start, height = rows.start, rows.size

        def body(r, c, carry):
            r = pl.ds(pl.multiple_of(r.start + start, ROWS), ROWS)
            total = whole[i][(*block, r, c)].astype(F32)
            for ref, lead, first in terms:
                total = total + ref[(*lead, pl.ds(pl.multiple_of(r.start - first, ROWS), ROWS), c)].astype(F32)
            whole[i][(*block, r, c)] = total.astype(BF16)
            return carry

        tiles(height, size[i][1], body)(0)

    def landed(ref, sem):
        pltpu.make_async_copy(ref, ref, sem).wait()

    def opposite1(i, j):
        landed(opp1[i].at[:, :, j], early1.at[i, j])

    def final1(i, j):
        landed(fin1[i].at[:, :, j], late1.at[i, j])

    def opposite2(i):
        landed(opp2[i], early2.at[i])

    def final2(i):
        landed(fin2[i], late2.at[i])

    def load(l, i, s):
        a, _ = ab(l)
        slab, rows = lax.rem(a + (1, 3, 0)[s], side), (low, high, everything)[s][i]
        where = (l, slab, slice(None), rows) if l == 0 else (l, slice(None), slab, rows)
        return pltpu.make_async_copy(g[i].at[where], whole[i].at[where], load_sem.at[i, s // 2])

    def states(i):
        return (
            pltpu.make_async_copy(m[i], new_m[i], state_sem.at[i, 0]),
            pltpu.make_async_copy(v[i], new_v[i], state_sem.at[i, 0]),
            *(pltpu.make_async_copy(w[i].at[l, x, y], own_w[i].at[l], state_sem.at[i, 1]) for l in layers),
        )

    barrier = pltpu.get_barrier_semaphore()
    for l in layers:
        a, b = ab(l)
        for step in (1, 3):
            pl.semaphore_signal(barrier, inc=1, device_id=device(l, a + step, b), device_id_type=MESH)
    for i in which:
        for l in layers:
            for s in (0, 1):
                load(l, i, s).start()
    pl.semaphore_wait(barrier, 4)

    def send_raw(i, j):
        for k in (0, 1, 2, 3):
            for l in layers:
                sum1(k, l, i, j).start()

    def pass_on1(i, j, first):
        if first:
            landed(whole[i].at[0, :2], load_sem.at[i, 0])
        opposite1(i, j)
        for l in layers:
            a, b = ab(l)
            for k in (0, 1):
                rows = (low, high)[k][i]
                add(i, rows, at(l, a + (1, 3)[k], b + j), (opp1[i], (l, k, j), rows.start))
                sum1(4 + k, l, i, j).start()

    def start2(i):
        landed(whole[i].at[0, :2], load_sem.at[i, 1])
        final1(i, 2)
        for l in layers:
            a, b = ab(l)
            add(i, everything[i], at(l, a, b + 2), (fin1[i], (l, 0, 2), 0), (fin1[i], (l, 1, 2), 0))
            sum2(0, l, i).start()
            sum2(1, l, i).start()
        final1(i, 1)
        final1(i, 3)
        for l in layers:
            a, b = ab(l)
            for k, j, rows in ((2, 1, high), (3, 3, low)):
                add(i, rows[i], at(l, a, b + j), (fin1[i], (l, 0, j), 0), (fin1[i], (l, 1, j), 0))
                sum2(k, l, i).start()

    def pass_on2(i):
        opposite2(i)
        for l in layers:
            a, b = ab(l)
            for k, j, rows in ((0, 1, low), (1, 3, high)):
                add(i, rows[i], at(l, a, b + j), (fin1[i], (l, 0, j), 0), (fin1[i], (l, 1, j), 0), (opp2[i], (l, k), rows[i].start))
                sum2(4 + k, l, i).start()

    def own(i, total):
        final1(i, 0)
        final2(i)
        for l in layers:

            def body(r, c, total, l=l):
                s = whole[i][l, x, y, r, c].astype(F32)
                for ref, lead in ((fin1[i], (l, 0, 0)), (fin1[i], (l, 1, 0)), (fin2[i], (l, 0)), (fin2[i], (l, 1))):
                    s = s + ref[(*lead, r, c)].astype(F32)
                s = s.astype(BF16)
                whole[i][l, x, y, r, c] = s
                s = s.astype(F32)
                return total + s * s

            total = tiles(*size[i], body)(total)
        return total

    def order(t):
        return (3 - t) * (4 - t) // 2 % side

    send_raw(0, 2)

    for i in which:
        for l in layers:
            load(l, i, 2).start()
        for one in states(i):
            one.start()

    def sums(t, first):
        for i in which:
            send_raw((i + 1) % 3, order(t) if i < 2 else order(t + 1))
            pass_on1(i, order(t), first)

    sums(0, True)

    def more(t, carry):
        sums(t, False)
        return carry

    lax.fori_loop(1, side - 1, more, 0)
    for i in which:
        if i < 2:
            send_raw(i + 1, 0)
        start2(i)
        if i > 0:
            pass_on2(i - 1)
        pass_on1(i, 0, False)
    pass_on2(2)

    total = jnp.zeros((ROWS, COLUMNS), F32)
    for i in which:
        total = own(i, total)
    total = jnp.sum(total.reshape(ROWS // 8, 8, COLUMNS), 0)
    mine[...] = functools.reduce(jnp.add, [total[:, 128 * q : 128 * (q + 1)] for q in range(COLUMNS // 128)])

    def sent():
        for i in which:
            landed(whole[i].at[:, :3], send1.at[i])
            landed(whole[i].at[:, :3, 0], send2.at[i])

    sent()

    def share(k):
        return remote(mine, squares.at[me], send_sq, recv_sq, {"dp": lax.rem(me + k, n)})

    lax.fori_loop(1, n, lambda k, c: (share(k).start(), c)[1], 0)
    squares[me] = mine[...]
    for i in which:
        landed(whole[i].at[0, :2], state_sem.at[i, 0])
        landed(own_w[i], state_sem.at[i, 1])
    landed(squares.at[: n - 1], recv_sq)
    total = functools.reduce(jnp.add, [squares[k] for k in range(n)])
    total = jnp.full((8, 128), jnp.sum(total), F32)
    factor = jnp.max(jnp.minimum(1.0, 0.5 * lax.rsqrt(total / count + 1e-30)))

    def update(l, i, rows):
        def body(r, c, carry):
            r = pl.ds(pl.multiple_of(r.start + rows.start, ROWS), ROWS)
            grad = whole[i][l, x, y, r, c].astype(F32) * factor
            old = own_w[i][l, r, c].astype(F32)
            moment = 0.9 * new_m[i][l, r, c] + 0.1 * grad
            square = 0.95 * new_v[i][l, r, c] + 0.05 * grad * grad
            step = moment * lax.rsqrt(square + 1e-8) + 0.1 * old
            whole[i][l, x, y, r, c] = (old - 0.02 * step).astype(BF16)
            new_m[i][l, r, c] = moment
            new_v[i][l, r, c] = square
            return carry

        tiles(rows.size, size[i][1], body)(0)

    def first(i, j):
        for k in (0, 1, 2, 3):
            for l in layers:
                gather1(k, l, i, j).start()

    def forward1(i, j):
        opposite1(i, j)
        for k in (4, 5):
            for l in layers:
                gather1(k, l, i, j).start()

    def forward2(i):
        opposite2(i)
        for k in (4, 5):
            for l in layers:
                gather2(k, l, i).start()

    for i in which:
        for l in layers:
            for rows, ks in ((low, (0, 3)), (high, (1, 2))):
                update(l, i, rows[i])
                for k in ks:
                    gather2(k, l, i).start()
                    if i == 0:
                        gather1(k, l, i, 0).start()
    forward2(0)
    first(1, 0)
    forward2(1)
    first(2, 0)
    forward1(0, 0)
    forward2(2)
    forward1(1, 0)

    def back(t):
        return t * (t + 1) // 2 % side

    def gathers(t, i):
        first(i, back(t))
        forward1((i + 2) % 3, back(t) if i > 0 else back(t - 1))

    for i in which:
        final2(i)
        gathers(1, i)

    def rest(t, carry):
        for i in which:
            gathers(t, i)
        return carry

    lax.fori_loop(2, side, rest, 0)
    forward1(2, 2)

    for i in which:
        for j in range(side):
            final1(i, j)
    sent()
    landed(squares.at[: n - 1], send_sq)


def drain(*refs):
    sources, targets, sem = refs[:9], refs[9:18], refs[18]
    copies = [pltpu.make_async_copy(s, t, sem.at[k]) for k, (s, t) in enumerate(zip(sources, targets, strict=True))]
    for copy in copies:
        copy.start()
    for copy in copies:
        copy.wait()


def solution(mesh):
    n = mesh.shape["dp"]
    side = math.isqrt(n)

    def step(*arrays):
        terms, weights, m, v = (arrays[i : i + 3] for i in (0, 3, 6, 9))
        count = n * sum(one.size for one in m)
        blocks = [one.shape for one in m]
        grid = [(l, side, side, r, c) for l, r, c in blocks]
        any_of = pl.BlockSpec(memory_space=pl.ANY)
        half = lambda *lead: [pltpu.VMEM((*lead, r // 2, c), BF16) for _, r, c in blocks]
        full = lambda *lead: [pltpu.VMEM((*lead, r, c), BF16) for _, r, c in blocks]
        dma = pltpu.SemaphoreType.DMA
        out = pl.pallas_call(
            functools.partial(kernel, n, count),
            out_shape=[pltpu.VMEM(one, BF16) for one in grid] + [pltpu.VMEM(one, F32) for one in blocks] * 2,
            in_specs=[any_of] * 12,
            out_specs=[pl.BlockSpec(memory_space=pltpu.VMEM)] * 9,
            scratch_shapes=[
                *half(2, 2, side),
                *full(2, 2, side),
                *half(2, 2),
                *full(2, 2),
                *full(2),
                pltpu.VMEM((n, 8, 128), F32),
                pltpu.VMEM((8, 128), F32),
                dma((3, 2)),
                dma((3, 2)),
                dma((3,)),
                dma((3,)),
                dma((3, side)),
                dma((3, side)),
                dma((3,)),
                dma((3,)),
                dma,
                dma,
            ],
            compiler_params=pltpu.CompilerParams(collective_id=0, has_side_effects=True, vmem_limit_bytes=25 << 20),
            name="step",
        )(
            *(t.reshape(one) for t, one in zip(terms, grid, strict=True)),
            *(t.reshape(one) for t, one in zip(weights, grid, strict=True)),
            *m,
            *v,
        )
        out = pl.pallas_call(
            drain,
            out_shape=[jax.ShapeDtypeStruct(one, BF16) for one in grid] + [jax.ShapeDtypeStruct(one, F32) for one in blocks] * 2,
            in_specs=[any_of] * 9,
            out_specs=[any_of] * 9,
            scratch_shapes=[dma((9,))],
            compiler_params=pltpu.CompilerParams(vmem_limit_bytes=1 << 20),
            name="drain",
        )(*(pltpu.with_memory_space_constraint(one, pltpu.VMEM) for one in out))
        return (*(one.reshape(w.shape) for one, w in zip(out[:3], weights, strict=True)), *out[3:])

    all_of, cut = P(None, None, None), P(None, "dp", None)
    return jax.shard_map(
        step,
        mesh=mesh,
        in_specs=(P(("rep", "dp"), None, None, None),) * 3 + (all_of,) * 3 + (cut,) * 6,
        out_specs=(P("rep", None, None),) * 3 + (P("rep", "dp", None),) * 6,
        check_vma=False,
    )
```

```python
import functools
import math

import jax
import jax.numpy as jnp
from jax import lax
from jax.experimental import pallas as pl
from jax.experimental.pallas import tpu as pltpu
from jax.sharding import PartitionSpec as P

MESH = pl.DeviceIdType.MESH
ROWS, COLUMNS = 16, 512
LATER = 10_000
BF16, F32 = jnp.bfloat16, jnp.float32


def tiles(rows, columns, body):
    across = columns // COLUMNS

    def one(t, carry):
        r, c = t // across, t % across
        return body(pl.ds(pl.multiple_of(r * ROWS, ROWS), ROWS), pl.ds(pl.multiple_of(c * COLUMNS, COLUMNS), COLUMNS), carry)

    return functools.partial(lax.fori_loop, 0, (rows // ROWS) * across, one)


def kernel(n, count, *refs):
    side = math.isqrt(n)
    g, w, m, v, whole, new_m, new_v = (refs[3 * i : 3 * i + 3] for i in range(7))
    opp1, fin1, opp2, fin2, own_w = (refs[21 + 3 * i : 24 + 3 * i] for i in range(5))
    squares, mine, load_sem, state_sem, send1, send2, early1, late1, early2, late2, send_sq, recv_sq = refs[36:]

    me = lax.axis_index("dp")
    x, y = me // side, me % side
    layers, which = (0, 1), (0, 1, 2)
    size = [(r.shape[-2], r.shape[-1]) for r in new_m]
    low = [pl.ds(0, r // 2) for r, _ in size]
    high = [pl.ds(r // 2, r // 2) for r, _ in size]
    everything = [pl.ds(0, r) for r, _ in size]

    def ab(l):
        return (x, y) if l == 0 else (y, x)

    def at(l, a, b):
        a, b = lax.rem(a, side), lax.rem(b, side)
        return (l, a, b) if l == 0 else (l, b, a)

    def device(l, a, b):
        _, p, q = at(l, a, b)
        return {"dp": p * side + q}

    def remote(src, dst, send, recv, target):
        return pltpu.make_async_remote_copy(src_ref=src, dst_ref=dst, send_sem=send, recv_sem=recv, device_id=target, device_id_type=MESH)

    def sum1(k, l, i, j):
        a, b = ab(l)
        step, rows = ((1, low), (3, high), (1, high), (3, low), (1, low), (3, high))[k]
        rows = rows[i]
        block = at(l, a + 2 if k < 2 else a + step, b + j)
        src = (g if k < 4 else whole)[i].at[(*block, rows)]
        way = k % 2
        dst = opp1[i].at[l, way, j] if k < 2 else fin1[i].at[l, way, j, rows]
        return remote(src, dst, send1.at[i], (early1 if k < 2 else late1).at[i, j], device(l, a + step, b))

    def sum2(k, l, i):
        a, b = ab(l)
        step, rows = ((1, low), (3, high), (1, high), (3, low), (1, low), (3, high))[k]
        rows = rows[i]
        src = whole[i].at[(*at(l, a, b + 2 if k < 2 else b + step), rows)]
        way = k % 2
        dst = opp2[i].at[l, way] if k < 2 else fin2[i].at[l, way, rows]
        return remote(src, dst, send2.at[i], (early2 if k < 2 else late2).at[i], device(l, a, b + step))

    def gather2(k, l, i):
        a, b = ab(l)
        step, rows, off = ((1, low, 0), (3, high, 0), (1, high, 0), (3, low, 0), (1, low, 3), (3, high, 1))[k]
        block = whole[i].at[(*at(l, a, b + off), rows[i])]
        return remote(block, block, send2.at[i], (early2 if k < 2 else late2).at[i], device(l, a, b + step))

    def gather1(k, l, i, j):
        a, b = ab(l)
        step, rows, off = ((1, low, 0), (3, high, 0), (1, high, 0), (3, low, 0), (1, low, 3), (3, high, 1))[k]
        block = whole[i].at[(*at(l, a + off, b + j), rows[i])]
        return remote(block, block, send1.at[i], (early1 if k < 2 else late1).at[i, j], device(l, a + step, b))

    def add(i, rows, block, *terms):
        start, height = rows.start, rows.size

        def body(r, c, carry):
            r = pl.ds(pl.multiple_of(r.start + start, ROWS), ROWS)
            total = whole[i][(*block, r, c)].astype(F32)
            for ref, lead, first in terms:
                total = total + ref[(*lead, pl.ds(pl.multiple_of(r.start - first, ROWS), ROWS), c)].astype(F32)
            whole[i][(*block, r, c)] = total.astype(BF16)
            return carry

        tiles(height, size[i][1], body)(0)

    def landed(ref, sem):
        pltpu.make_async_copy(ref, ref, sem).wait()

    def opposite1(i, j):
        landed(opp1[i].at[:, :, j], early1.at[i, j])

    def final1(i, j):
        landed(fin1[i].at[:, :, j], late1.at[i, j])

    def opposite2(i):
        landed(opp2[i], early2.at[i])

    def final2(i):
        landed(fin2[i], late2.at[i])

    def load(l, i, s):
        a, _ = ab(l)
        slab, rows = lax.rem(a + (1, 3, 0)[s], side), (low, high, everything)[s][i]
        where = (l, slab, slice(None), rows) if l == 0 else (l, slice(None), slab, rows)
        return pltpu.make_async_copy(g[i].at[where], whole[i].at[where], load_sem.at[i, s // 2])

    def states(i):
        return (
            pltpu.make_async_copy(m[i], new_m[i], state_sem.at[i, 0]),
            pltpu.make_async_copy(v[i], new_v[i], state_sem.at[i, 0]),
            *(pltpu.make_async_copy(w[i].at[l, x, y], own_w[i].at[l], state_sem.at[i, 1]) for l in layers),
        )

    barrier = pltpu.get_barrier_semaphore()
    for l in layers:
        a, b = ab(l)
        for step in (1, 3):
            pl.semaphore_signal(barrier, inc=1, device_id=device(l, a + step, b), device_id_type=MESH)
    for i in which:
        for l in layers:
            for s in (0, 1):
                load(l, i, s).start()
    pl.semaphore_wait(barrier, 4)

    @pl.when(lax.rem(lax.axis_index("rep"), 2) == 0)
    def _():
        pl.delay(LATER)

    def send_raw(i, j):
        for k in (0, 1, 2, 3):
            for l in layers:
                sum1(k, l, i, j).start()

    def pass_on1(i, j, first):
        if first:
            landed(whole[i].at[0, :2], load_sem.at[i, 0])
        opposite1(i, j)
        for l in layers:
            a, b = ab(l)
            for k in (0, 1):
                rows = (low, high)[k][i]
                add(i, rows, at(l, a + (1, 3)[k], b + j), (opp1[i], (l, k, j), rows.start))
                sum1(4 + k, l, i, j).start()

    def start2(i):
        landed(whole[i].at[0, :2], load_sem.at[i, 1])
        final1(i, 2)
        for l in layers:
            a, b = ab(l)
            add(i, everything[i], at(l, a, b + 2), (fin1[i], (l, 0, 2), 0), (fin1[i], (l, 1, 2), 0))
            sum2(0, l, i).start()
            sum2(1, l, i).start()
        final1(i, 1)
        final1(i, 3)
        for l in layers:
            a, b = ab(l)
            for k, j, rows in ((2, 1, high), (3, 3, low)):
                add(i, rows[i], at(l, a, b + j), (fin1[i], (l, 0, j), 0), (fin1[i], (l, 1, j), 0))
                sum2(k, l, i).start()

    def pass_on2(i):
        opposite2(i)
        for l in layers:
            a, b = ab(l)
            for k, j, rows in ((0, 1, low), (1, 3, high)):
                add(i, rows[i], at(l, a, b + j), (fin1[i], (l, 0, j), 0), (fin1[i], (l, 1, j), 0), (opp2[i], (l, k), rows[i].start))
                sum2(4 + k, l, i).start()

    def own(i, total):
        final1(i, 0)
        final2(i)
        for l in layers:

            def body(r, c, total, l=l):
                s = whole[i][l, x, y, r, c].astype(F32)
                for ref, lead in ((fin1[i], (l, 0, 0)), (fin1[i], (l, 1, 0)), (fin2[i], (l, 0)), (fin2[i], (l, 1))):
                    s = s + ref[(*lead, r, c)].astype(F32)
                s = s.astype(BF16)
                whole[i][l, x, y, r, c] = s
                s = s.astype(F32)
                return total + s * s

            total = tiles(*size[i], body)(total)
        return total

    def order(t):
        return (3 - t) * (4 - t) // 2 % side

    send_raw(0, 2)

    for i in which:
        for l in layers:
            load(l, i, 2).start()
        for one in states(i):
            one.start()

    def sums(t, first):
        for i in which:
            send_raw((i + 1) % 3, order(t) if i < 2 else order(t + 1))
            pass_on1(i, order(t), first)

    sums(0, True)

    def more(t, carry):
        sums(t, False)
        return carry

    lax.fori_loop(1, side - 1, more, 0)
    for i in which:
        if i < 2:
            send_raw(i + 1, 0)
        start2(i)
        if i > 0:
            pass_on2(i - 1)
        pass_on1(i, 0, False)
    pass_on2(2)

    total = jnp.zeros((ROWS, COLUMNS), F32)
    for i in which:
        total = own(i, total)
    total = jnp.sum(total.reshape(ROWS // 8, 8, COLUMNS), 0)
    mine[...] = functools.reduce(jnp.add, [total[:, 128 * q : 128 * (q + 1)] for q in range(COLUMNS // 128)])

    def sent():
        for i in which:
            landed(whole[i].at[:, :3], send1.at[i])
            landed(whole[i].at[:, :3, 0], send2.at[i])

    sent()

    def share(k):
        return remote(mine, squares.at[me], send_sq, recv_sq, {"dp": lax.rem(me + k, n)})

    lax.fori_loop(1, n, lambda k, c: (share(k).start(), c)[1], 0)
    squares[me] = mine[...]
    for i in which:
        landed(whole[i].at[0, :2], state_sem.at[i, 0])
        landed(own_w[i], state_sem.at[i, 1])
    landed(squares.at[: n - 1], recv_sq)
    total = functools.reduce(jnp.add, [squares[k] for k in range(n)])
    total = jnp.full((8, 128), jnp.sum(total), F32)
    factor = jnp.max(jnp.minimum(1.0, 0.5 * lax.rsqrt(total / count + 1e-30)))

    def update(l, i, rows):
        def body(r, c, carry):
            r = pl.ds(pl.multiple_of(r.start + rows.start, ROWS), ROWS)
            grad = whole[i][l, x, y, r, c].astype(F32) * factor
            old = own_w[i][l, r, c].astype(F32)
            moment = 0.9 * new_m[i][l, r, c] + 0.1 * grad
            square = 0.95 * new_v[i][l, r, c] + 0.05 * grad * grad
            step = moment * lax.rsqrt(square + 1e-8) + 0.1 * old
            whole[i][l, x, y, r, c] = (old - 0.02 * step).astype(BF16)
            new_m[i][l, r, c] = moment
            new_v[i][l, r, c] = square
            return carry

        tiles(rows.size, size[i][1], body)(0)

    def first(i, j):
        for k in (0, 1, 2, 3):
            for l in layers:
                gather1(k, l, i, j).start()

    def forward1(i, j):
        opposite1(i, j)
        for k in (4, 5):
            for l in layers:
                gather1(k, l, i, j).start()

    def forward2(i):
        opposite2(i)
        for k in (4, 5):
            for l in layers:
                gather2(k, l, i).start()

    for i in which:
        for l in layers:
            for rows, ks in ((low, (0, 3)), (high, (1, 2))):
                update(l, i, rows[i])
                for k in ks:
                    gather2(k, l, i).start()
                    if i == 0:
                        gather1(k, l, i, 0).start()
    forward2(0)
    first(1, 0)
    forward2(1)
    first(2, 0)
    forward1(0, 0)
    forward2(2)
    forward1(1, 0)

    def back(t):
        return t * (t + 1) // 2 % side

    def gathers(t, i):
        first(i, back(t))
        forward1((i + 2) % 3, back(t) if i > 0 else back(t - 1))

    for i in which:
        final2(i)
        gathers(1, i)

    def rest(t, carry):
        for i in which:
            gathers(t, i)
        return carry

    lax.fori_loop(2, side, rest, 0)
    forward1(2, 2)

    for i in which:
        for j in range(side):
            final1(i, j)
    sent()
    landed(squares.at[: n - 1], send_sq)


def drain(*refs):
    sources, targets, sem = refs[:9], refs[9:18], refs[18]
    copies = [pltpu.make_async_copy(s, t, sem.at[k]) for k, (s, t) in enumerate(zip(sources, targets, strict=True))]
    for copy in copies:
        copy.start()
    for copy in copies:
        copy.wait()


def solution(mesh):
    n = mesh.shape["dp"]
    side = math.isqrt(n)

    def step(*arrays):
        terms, weights, m, v = (arrays[i : i + 3] for i in (0, 3, 6, 9))
        count = n * sum(one.size for one in m)
        blocks = [one.shape for one in m]
        grid = [(l, side, side, r, c) for l, r, c in blocks]
        any_of = pl.BlockSpec(memory_space=pl.ANY)
        half = lambda *lead: [pltpu.VMEM((*lead, r // 2, c), BF16) for _, r, c in blocks]
        full = lambda *lead: [pltpu.VMEM((*lead, r, c), BF16) for _, r, c in blocks]
        dma = pltpu.SemaphoreType.DMA
        out = pl.pallas_call(
            functools.partial(kernel, n, count),
            out_shape=[pltpu.VMEM(one, BF16) for one in grid] + [pltpu.VMEM(one, F32) for one in blocks] * 2,
            in_specs=[any_of] * 12,
            out_specs=[pl.BlockSpec(memory_space=pltpu.VMEM)] * 9,
            scratch_shapes=[
                *half(2, 2, side),
                *full(2, 2, side),
                *half(2, 2),
                *full(2, 2),
                *full(2),
                pltpu.VMEM((n, 8, 128), F32),
                pltpu.VMEM((8, 128), F32),
                dma((3, 2)),
                dma((3, 2)),
                dma((3,)),
                dma((3,)),
                dma((3, side)),
                dma((3, side)),
                dma((3,)),
                dma((3,)),
                dma,
                dma,
            ],
            compiler_params=pltpu.CompilerParams(collective_id=0, has_side_effects=True, vmem_limit_bytes=25 << 20),
            name="step",
        )(
            *(t.reshape(one) for t, one in zip(terms, grid, strict=True)),
            *(t.reshape(one) for t, one in zip(weights, grid, strict=True)),
            *m,
            *v,
        )
        out = pl.pallas_call(
            drain,
            out_shape=[jax.ShapeDtypeStruct(one, BF16) for one in grid] + [jax.ShapeDtypeStruct(one, F32) for one in blocks] * 2,
            in_specs=[any_of] * 9,
            out_specs=[any_of] * 9,
            scratch_shapes=[dma((9,))],
            compiler_params=pltpu.CompilerParams(vmem_limit_bytes=1 << 20),
            name="drain",
        )(*(pltpu.with_memory_space_constraint(one, pltpu.VMEM) for one in out))
        return (*(one.reshape(w.shape) for one, w in zip(out[:3], weights, strict=True)), *out[3:])

    all_of, cut = P(None, None, None), P(None, "dp", None)
    return jax.shard_map(
        step,
        mesh=mesh,
        in_specs=(P(("rep", "dp"), None, None, None),) * 3 + (all_of,) * 3 + (cut,) * 6,
        out_specs=(P("rep", None, None),) * 3 + (P("rep", "dp", None),) * 6,
        check_vma=False,
    )
```

```python
import functools
import math

import jax
import jax.numpy as jnp
from jax import lax
from jax.experimental import pallas as pl
from jax.experimental.pallas import tpu as pltpu
from jax.sharding import PartitionSpec as P

MESH = pl.DeviceIdType.MESH
LAYERS = (0, 1)
ROWS, COLUMNS = 16, 512
LATER = 10_000
BF16, F32 = jnp.bfloat16, jnp.float32


def tiles(rows, columns, body):
    across = columns // COLUMNS

    def one(t, carry):
        r, c = t // across, t % across
        return body(pl.ds(pl.multiple_of(r * ROWS, ROWS), ROWS), pl.ds(pl.multiple_of(c * COLUMNS, COLUMNS), COLUMNS), carry)

    return functools.partial(lax.fori_loop, 0, (rows // ROWS) * across, one)


class Torus:
    def __init__(self, n):
        self.side = math.isqrt(n)
        self.me = lax.axis_index("dp")
        self.x, self.y = self.me // self.side, self.me % self.side

    def ab(self, l):
        return (self.x, self.y) if l == 0 else (self.y, self.x)

    def at(self, l, a, b):
        a, b = lax.rem(a, self.side), lax.rem(b, self.side)
        return (l, a, b) if l == 0 else (l, b, a)

    def device(self, l, a, b):
        _, p, q = self.at(l, a, b)
        return {"dp": p * self.side + q}

    def greet(self):
        barrier = pltpu.get_barrier_semaphore()
        for l in LAYERS:
            a, b = self.ab(l)
            for step in (1, 3):
                pl.semaphore_signal(barrier, inc=1, device_id=self.device(l, a + step, b), device_id_type=MESH)
        return lambda: pl.semaphore_wait(barrier, 4)


def remote(src, dst, send, recv, target):
    return pltpu.make_async_remote_copy(src_ref=src, dst_ref=dst, send_sem=send, recv_sem=recv, device_id=target, device_id_type=MESH)


def landed(ref, sem):
    pltpu.make_async_copy(ref, ref, sem).wait()


class Gather:
    def __init__(self, torus, whole, send1, send2, early1, late1, early2, late2):
        self.torus, self.whole = torus, whole
        self.send1, self.send2, self.early1, self.late1, self.early2, self.late2 = send1, send2, early1, late1, early2, late2
        rows = whole.shape[-2]
        low, high = pl.ds(0, rows // 2), pl.ds(rows // 2, rows // 2)
        self.kinds = ((1, low, 0), (3, high, 0), (1, high, 0), (3, low, 0), (1, low, 3), (3, high, 1))

    def copy2(self, k, l):
        a, b = self.torus.ab(l)
        step, rows, off = self.kinds[k]
        block = self.whole.at[(*self.torus.at(l, a, b + off), rows)]
        return remote(block, block, self.send2, self.early2 if k < 2 else self.late2, self.torus.device(l, a, b + step))

    def copy1(self, k, l, j):
        a, b = self.torus.ab(l)
        step, rows, off = self.kinds[k]
        block = self.whole.at[(*self.torus.at(l, a + off, b + j), rows)]
        return remote(block, block, self.send1, (self.early1 if k < 2 else self.late1).at[j], self.torus.device(l, a + step, b))

    def first2(self):
        for k in (0, 1, 2, 3):
            for l in LAYERS:
                self.copy2(k, l).start()

    def forward2(self):
        landed(self.whole.at[0, 0, :2], self.early2)
        for k in (4, 5):
            for l in LAYERS:
                self.copy2(k, l).start()

    def final2(self):
        landed(self.whole.at[0, 0], self.late2)

    def first1(self, j):
        for k in (0, 1, 2, 3):
            for l in LAYERS:
                self.copy1(k, l, j).start()

    def forward1(self, j):
        landed(self.whole.at[0, 0, :2], self.early1.at[j])
        for k in (4, 5):
            for l in LAYERS:
                self.copy1(k, l, j).start()

    def finish(self):
        for j in range(self.torus.side):
            landed(self.whole.at[0, 0], self.late1.at[j])
        self.sent()

    def sent(self):
        landed(self.whole.at[:, :3], self.send1)
        landed(self.whole.at[:, :3, 0], self.send2)


def back(t, side):
    return t * (t + 1) // 2 % side


def kernel(n, count, *refs):
    side = math.isqrt(n)
    g, w, m, v = (refs[3 * i : 3 * i + 3] for i in range(4))
    new_m, new_v = refs[14:17], refs[17:20]
    left = refs[20]
    whole = (*refs[12:14], refs[21])
    opp1, fin1, opp2, fin2, own_w = (refs[22 + 3 * i : 25 + 3 * i] for i in range(5))
    squares, mine, load_sem, state_sem, send1, send2, early1, late1, early2, late2, send_sq, recv_sq = refs[37:]

    torus = Torus(n)
    me, x, y, ab, at, device = torus.me, torus.x, torus.y, torus.ab, torus.at, torus.device
    layers, which = LAYERS, (0, 1, 2)
    size = [(r.shape[-2], r.shape[-1]) for r in new_m]
    low = [pl.ds(0, r // 2) for r, _ in size]
    high = [pl.ds(r // 2, r // 2) for r, _ in size]
    everything = [pl.ds(0, r) for r, _ in size]

    def sum1(k, l, i, j):
        a, b = ab(l)
        step, rows = ((1, low), (3, high), (1, high), (3, low), (1, low), (3, high))[k]
        rows = rows[i]
        block = at(l, a + 2 if k < 2 else a + step, b + j)
        src = (g if k < 4 else whole)[i].at[(*block, rows)]
        way = k % 2
        dst = opp1[i].at[l, way, j] if k < 2 else fin1[i].at[l, way, j, rows]
        return remote(src, dst, send1.at[i], (early1 if k < 2 else late1).at[i, j], device(l, a + step, b))

    def sum2(k, l, i):
        a, b = ab(l)
        step, rows = ((1, low), (3, high), (1, high), (3, low), (1, low), (3, high))[k]
        rows = rows[i]
        src = whole[i].at[(*at(l, a, b + 2 if k < 2 else b + step), rows)]
        way = k % 2
        dst = opp2[i].at[l, way] if k < 2 else fin2[i].at[l, way, rows]
        return remote(src, dst, send2.at[i], (early2 if k < 2 else late2).at[i], device(l, a, b + step))

    def add(i, rows, block, *terms):
        start, height = rows.start, rows.size

        def body(r, c, carry):
            r = pl.ds(pl.multiple_of(r.start + start, ROWS), ROWS)
            total = whole[i][(*block, r, c)].astype(F32)
            for ref, lead, first in terms:
                total = total + ref[(*lead, pl.ds(pl.multiple_of(r.start - first, ROWS), ROWS), c)].astype(F32)
            whole[i][(*block, r, c)] = total.astype(BF16)
            return carry

        tiles(height, size[i][1], body)(0)

    def opposite1(i, j):
        landed(opp1[i].at[:, :, j], early1.at[i, j])

    def final1(i, j):
        landed(fin1[i].at[:, :, j], late1.at[i, j])

    def opposite2(i):
        landed(opp2[i], early2.at[i])

    def final2(i):
        landed(fin2[i], late2.at[i])

    def load(l, i, s):
        a, _ = ab(l)
        slab, rows = lax.rem(a + (1, 3, 0)[s], side), (low, high, everything)[s][i]
        where = (l, slab, slice(None), rows) if l == 0 else (l, slice(None), slab, rows)
        return pltpu.make_async_copy(g[i].at[where], whole[i].at[where], load_sem.at[i, s // 2])

    def states(i):
        return (
            pltpu.make_async_copy(m[i], new_m[i], state_sem.at[i, 0]),
            pltpu.make_async_copy(v[i], new_v[i], state_sem.at[i, 0]),
            *(pltpu.make_async_copy(w[i].at[l, x, y], own_w[i].at[l], state_sem.at[i, 1]) for l in layers),
        )

    wait_for_neighbours = torus.greet()
    for i in which:
        for l in layers:
            for s in (0, 1):
                load(l, i, s).start()
    wait_for_neighbours()

    @pl.when(lax.rem(lax.axis_index("rep"), 2) == 0)
    def _():
        pl.delay(LATER)

    def send_raw(i, j):
        for k in (0, 1, 2, 3):
            for l in layers:
                sum1(k, l, i, j).start()

    def pass_on1(i, j, first):
        if first:
            landed(whole[i].at[0, :2], load_sem.at[i, 0])
        opposite1(i, j)
        for l in layers:
            a, b = ab(l)
            for k in (0, 1):
                rows = (low, high)[k][i]
                add(i, rows, at(l, a + (1, 3)[k], b + j), (opp1[i], (l, k, j), rows.start))
                sum1(4 + k, l, i, j).start()

    def start2(i):
        landed(whole[i].at[0, :2], load_sem.at[i, 1])
        final1(i, 2)
        for l in layers:
            a, b = ab(l)
            add(i, everything[i], at(l, a, b + 2), (fin1[i], (l, 0, 2), 0), (fin1[i], (l, 1, 2), 0))
            sum2(0, l, i).start()
            sum2(1, l, i).start()
        final1(i, 1)
        final1(i, 3)
        for l in layers:
            a, b = ab(l)
            for k, j, rows in ((2, 1, high), (3, 3, low)):
                add(i, rows[i], at(l, a, b + j), (fin1[i], (l, 0, j), 0), (fin1[i], (l, 1, j), 0))
                sum2(k, l, i).start()

    def pass_on2(i):
        opposite2(i)
        for l in layers:
            a, b = ab(l)
            for k, j, rows in ((0, 1, low), (1, 3, high)):
                add(i, rows[i], at(l, a, b + j), (fin1[i], (l, 0, j), 0), (fin1[i], (l, 1, j), 0), (opp2[i], (l, k), rows[i].start))
                sum2(4 + k, l, i).start()

    def own(i, total):
        final1(i, 0)
        final2(i)
        for l in layers:

            def body(r, c, total, l=l):
                s = whole[i][l, x, y, r, c].astype(F32)
                for ref, lead in ((fin1[i], (l, 0, 0)), (fin1[i], (l, 1, 0)), (fin2[i], (l, 0)), (fin2[i], (l, 1))):
                    s = s + ref[(*lead, r, c)].astype(F32)
                s = s.astype(BF16)
                whole[i][l, x, y, r, c] = s
                s = s.astype(F32)
                return total + s * s

            total = tiles(*size[i], body)(total)
        return total

    def order(t):
        return (3 - t) * (4 - t) // 2 % side

    send_raw(0, 2)

    for i in which:
        for l in layers:
            load(l, i, 2).start()
        for one in states(i):
            one.start()

    def sums(t, first):
        for i in which:
            send_raw((i + 1) % 3, order(t) if i < 2 else order(t + 1))
            pass_on1(i, order(t), first)

    sums(0, True)

    def more(t, carry):
        sums(t, False)
        return carry

    lax.fori_loop(1, side - 1, more, 0)
    for i in which:
        if i < 2:
            send_raw(i + 1, 0)
        start2(i)
        if i > 0:
            pass_on2(i - 1)
        pass_on1(i, 0, False)
    pass_on2(2)

    total = jnp.zeros((ROWS, COLUMNS), F32)
    for i in which:
        total = own(i, total)
    total = jnp.sum(total.reshape(ROWS // 8, 8, COLUMNS), 0)
    mine[...] = functools.reduce(jnp.add, [total[:, 128 * q : 128 * (q + 1)] for q in range(COLUMNS // 128)])

    gathers = [Gather(torus, whole[i], *(sem.at[i] for sem in (send1, send2, early1, late1, early2, late2))) for i in which]
    for one in gathers:
        one.sent()

    def share(k):
        return remote(mine, squares.at[me], send_sq, recv_sq, {"dp": lax.rem(me + k, n)})

    lax.fori_loop(1, n, lambda k, c: (share(k).start(), c)[1], 0)
    squares[me] = mine[...]
    for i in which:
        landed(whole[i].at[0, :2], state_sem.at[i, 0])
        landed(own_w[i], state_sem.at[i, 1])
    landed(squares.at[: n - 1], recv_sq)
    total = functools.reduce(jnp.add, [squares[k] for k in range(n)])
    total = jnp.full((8, 128), jnp.sum(total), F32)
    factor = jnp.max(jnp.minimum(1.0, 0.5 * lax.rsqrt(total / count + 1e-30)))

    def update(l, i, rows):
        def body(r, c, carry):
            r = pl.ds(pl.multiple_of(r.start + rows.start, ROWS), ROWS)
            grad = whole[i][l, x, y, r, c].astype(F32) * factor
            old = own_w[i][l, r, c].astype(F32)
            moment = 0.9 * new_m[i][l, r, c] + 0.1 * grad
            square = 0.95 * new_v[i][l, r, c] + 0.05 * grad * grad
            step = moment * lax.rsqrt(square + 1e-8) + 0.1 * old
            new = (old - 0.02 * step).astype(BF16)
            if i < 2:
                whole[i][l, x, y, r, c] = new
            else:
                left[l, r, c] = new
            new_m[i][l, r, c] = moment
            new_v[i][l, r, c] = square
            return carry

        tiles(rows.size, size[i][1], body)(0)

    one, two, _ = gathers
    for l in layers:
        for rows, ks in ((low, (0, 3)), (high, (1, 2))):
            update(l, 0, rows[0])
            for k in ks:
                one.copy2(k, l).start()
                one.copy1(k, l, 0).start()
    for l in layers:
        update(l, 1, everything[1])
    two.first2()
    one.forward2()
    two.first1(0)
    for l in layers:
        update(l, 2, everything[2])
    two.forward2()
    one.forward1(0)
    one.final2()
    one.first1(1)
    two.forward1(0)
    two.final2()
    two.first1(1)
    one.forward1(1)

    def rest(t, carry):
        one.first1(back(t, side))
        two.forward1(back(t - 1, side))
        two.first1(back(t, side))
        one.forward1(back(t, side))
        return carry

    lax.fori_loop(2, side, rest, 0)
    two.forward1(back(side - 1, side))
    one.finish()
    two.finish()
    landed(squares.at[: n - 1], send_sq)


def gather_last(n, block, whole, send1, send2, early1, late1, early2, late2, own_sem):
    torus = Torus(n)
    wait_for_neighbours = torus.greet()
    own = pltpu.make_async_copy(block, whole.at[:, torus.x, torus.y], own_sem)
    own.start()
    wait_for_neighbours()
    own.wait()
    one = Gather(torus, whole, send1, send2, early1, late1, early2, late2)
    one.first2()
    one.first1(0)
    one.forward2()
    one.forward1(0)
    one.final2()
    one.first1(1)

    def rest(t, carry):
        one.first1(back(t, torus.side))
        one.forward1(back(t - 1, torus.side))
        return carry

    lax.fori_loop(2, torus.side, rest, 0)
    one.forward1(back(torus.side - 1, torus.side))
    one.finish()


def drain(*refs):
    sources, targets, sem = refs[: len(refs) // 2], refs[len(refs) // 2 : -1], refs[-1]
    copies = [pltpu.make_async_copy(s, t, sem.at[k]) for k, (s, t) in enumerate(zip(sources, targets, strict=True))]
    for copy in copies:
        copy.start()
    for copy in copies:
        copy.wait()


def solution(mesh):
    n = mesh.shape["dp"]
    side = math.isqrt(n)

    def step(*arrays):
        terms, weights, m, v = (arrays[i : i + 3] for i in (0, 3, 6, 9))
        count = n * sum(one.size for one in m)
        blocks = [one.shape for one in m]
        grid = [(l, side, side, r, c) for l, r, c in blocks]
        any_of = pl.BlockSpec(memory_space=pl.ANY)
        half = lambda *lead: [pltpu.VMEM((*lead, r // 2, c), BF16) for _, r, c in blocks]
        full = lambda *lead: [pltpu.VMEM((*lead, r, c), BF16) for _, r, c in blocks]
        dma = pltpu.SemaphoreType.DMA
        in_vmem = pl.BlockSpec(memory_space=pltpu.VMEM)

        def copy_out(arrays, name):
            return pl.pallas_call(
                drain,
                out_shape=[pltpu.HBM(one.shape, one.dtype) for one in arrays],
                in_specs=[any_of] * len(arrays),
                out_specs=[any_of] * len(arrays),
                scratch_shapes=[dma((len(arrays),))],
                compiler_params=pltpu.CompilerParams(vmem_limit_bytes=1 << 20),
                name=name,
            )(*(pltpu.with_memory_space_constraint(one, pltpu.VMEM) for one in arrays))

        out = pl.pallas_call(
            functools.partial(kernel, n, count),
            out_shape=[pltpu.VMEM(one, BF16) for one in grid[:2]] + [pltpu.VMEM(one, F32) for one in blocks] * 2 + [pltpu.VMEM(blocks[2], BF16)],
            in_specs=[any_of] * 12,
            out_specs=[in_vmem] * 9,
            scratch_shapes=[
                pltpu.VMEM(grid[2], BF16),
                *half(2, 2, side),
                *full(2, 2, side),
                *half(2, 2),
                *full(2, 2),
                *full(2),
                pltpu.VMEM((n, 8, 128), F32),
                pltpu.VMEM((8, 128), F32),
                dma((3, 2)),
                dma((3, 2)),
                dma((3,)),
                dma((3,)),
                dma((3, side)),
                dma((3, side)),
                dma((3,)),
                dma((3,)),
                dma,
                dma,
            ],
            compiler_params=pltpu.CompilerParams(collective_id=0, has_side_effects=True, vmem_limit_bytes=33 << 20),
            name="step",
        )(
            *(t.reshape(one) for t, one in zip(terms, grid, strict=True)),
            *(t.reshape(one) for t, one in zip(weights, grid, strict=True)),
            *m,
            *v,
        )
        gate, up, *moments, left = copy_out(out, "copy_out")
        (last,) = pl.pallas_call(
            functools.partial(gather_last, n),
            out_shape=[pltpu.VMEM(grid[2], BF16)],
            in_specs=[any_of],
            out_specs=[in_vmem],
            scratch_shapes=[dma, dma, dma((side,)), dma((side,)), dma, dma, dma],
            compiler_params=pltpu.CompilerParams(collective_id=1, has_side_effects=True, vmem_limit_bytes=1 << 20),
            name="gather_last",
        )(pltpu.with_memory_space_constraint(left, pltpu.HBM))
        (down,) = copy_out([last], "copy_last_out")
        return (*(one.reshape(w.shape) for one, w in zip((gate, up, down), weights, strict=True)), *moments)

    all_of, cut = P(None, None, None), P(None, "dp", None)
    return jax.shard_map(
        step,
        mesh=mesh,
        in_specs=(P(("rep", "dp"), None, None, None),) * 3 + (all_of,) * 3 + (cut,) * 6,
        out_specs=(P("rep", None, None),) * 3 + (P("rep", "dp", None),) * 6,
        check_vma=False,
    )
```

```python
import functools
import math

import jax
import jax.numpy as jnp
from jax import lax
from jax.experimental import pallas as pl
from jax.experimental.pallas import tpu as pltpu
from jax.sharding import PartitionSpec as P

MESH = pl.DeviceIdType.MESH
LAYERS = (0, 1)
ROWS, COLUMNS = 16, 512
LATER = 10_000
BF16, F32 = jnp.bfloat16, jnp.float32


def tiles(rows, columns, body):
    across = columns // COLUMNS

    def one(t, carry):
        r, c = t // across, t % across
        return body(pl.ds(pl.multiple_of(r * ROWS, ROWS), ROWS), pl.ds(pl.multiple_of(c * COLUMNS, COLUMNS), COLUMNS), carry)

    return functools.partial(lax.fori_loop, 0, (rows // ROWS) * across, one)


class Torus:
    def __init__(self, n):
        self.side = math.isqrt(n)
        self.me = lax.axis_index("dp")
        self.x, self.y = self.me // self.side, self.me % self.side

    def ab(self, l):
        return (self.x, self.y) if l == 0 else (self.y, self.x)

    def at(self, l, a, b):
        a, b = lax.rem(a, self.side), lax.rem(b, self.side)
        return (l, a, b) if l == 0 else (l, b, a)

    def device(self, l, a, b):
        _, p, q = self.at(l, a, b)
        return {"dp": p * self.side + q}

    def greet(self):
        barrier = pltpu.get_barrier_semaphore()
        for l in LAYERS:
            a, b = self.ab(l)
            for step in (1, 3):
                pl.semaphore_signal(barrier, inc=1, device_id=self.device(l, a + step, b), device_id_type=MESH)
        return lambda: pl.semaphore_wait(barrier, 4)


def remote(src, dst, send, recv, target):
    return pltpu.make_async_remote_copy(src_ref=src, dst_ref=dst, send_sem=send, recv_sem=recv, device_id=target, device_id_type=MESH)


def landed(ref, sem):
    pltpu.make_async_copy(ref, ref, sem).wait()


class Gather:
    def __init__(self, torus, whole, send1, send2, early1, late1, early2, late2):
        self.torus, self.whole = torus, whole
        self.send1, self.send2, self.early1, self.late1, self.early2, self.late2 = send1, send2, early1, late1, early2, late2
        rows = whole.shape[-2]
        low, high = pl.ds(0, rows // 2), pl.ds(rows // 2, rows // 2)
        self.kinds = ((1, low, 0), (3, high, 0), (1, high, 0), (3, low, 0), (1, low, 3), (3, high, 1))

    def copy2(self, k, l):
        a, b = self.torus.ab(l)
        step, rows, off = self.kinds[k]
        block = self.whole.at[(*self.torus.at(l, a, b + off), rows)]
        return remote(block, block, self.send2, self.early2 if k < 2 else self.late2, self.torus.device(l, a, b + step))

    def copy1(self, k, l, j):
        a, b = self.torus.ab(l)
        step, rows, off = self.kinds[k]
        block = self.whole.at[(*self.torus.at(l, a + off, b + j), rows)]
        return remote(block, block, self.send1, (self.early1 if k < 2 else self.late1).at[j], self.torus.device(l, a + step, b))

    def first2(self):
        for k in (0, 1, 2, 3):
            for l in LAYERS:
                self.copy2(k, l).start()

    def forward2(self):
        landed(self.whole.at[0, 0, :2], self.early2)
        for k in (4, 5):
            for l in LAYERS:
                self.copy2(k, l).start()

    def final2(self):
        landed(self.whole.at[0, 0], self.late2)

    def first1(self, j):
        for k in (0, 1, 2, 3):
            for l in LAYERS:
                self.copy1(k, l, j).start()

    def forward1(self, j):
        landed(self.whole.at[0, 0, :2], self.early1.at[j])
        for k in (4, 5):
            for l in LAYERS:
                self.copy1(k, l, j).start()

    def finish(self):
        for j in range(self.torus.side):
            landed(self.whole.at[0, 0], self.late1.at[j])
        self.sent()

    def sent(self):
        landed(self.whole.at[:, :3], self.send1)
        landed(self.whole.at[:, :3, 0], self.send2)


def back(t, side):
    return t * (t + 1) // 2 % side


def kernel(n, count, *refs):
    side = math.isqrt(n)
    g, w, m, v = (refs[3 * i : 3 * i + 3] for i in range(4))
    new_m, new_v = refs[14:17], refs[17:20]
    left = refs[20]
    whole = (*refs[12:14], refs[21])
    opp1, fin1, opp2, fin2, own_w = (refs[22 + 3 * i : 25 + 3 * i] for i in range(5))
    squares, mine, load_sem, state_sem, send1, send2, early1, late1, early2, late2, send_sq, recv_sq, stage_sem = refs[37:]

    torus = Torus(n)
    me, x, y, ab, at, device = torus.me, torus.x, torus.y, torus.ab, torus.at, torus.device
    layers, which = LAYERS, (0, 1, 2)
    size = [(r.shape[-2], r.shape[-1]) for r in new_m]
    low = [pl.ds(0, r // 2) for r, _ in size]
    high = [pl.ds(r // 2, r // 2) for r, _ in size]
    everything = [pl.ds(0, r) for r, _ in size]

    def sum1(k, l, i, j, staged=False):
        a, b = ab(l)
        step, rows = ((1, low), (3, high), (1, high), (3, low), (1, low), (3, high))[k]
        rows = rows[i]
        block = at(l, a + 2 if k < 2 else a + step, b + j)
        src = (whole if staged or k > 3 else g)[i].at[(*block, rows)]
        way = k % 2
        dst = opp1[i].at[l, way, j] if k < 2 else fin1[i].at[l, way, j, rows]
        return remote(src, dst, send1.at[i], (early1 if k < 2 else late1).at[i, j], device(l, a + step, b))

    def sum2(k, l, i):
        a, b = ab(l)
        step, rows = ((1, low), (3, high), (1, high), (3, low), (1, low), (3, high))[k]
        rows = rows[i]
        src = whole[i].at[(*at(l, a, b + 2 if k < 2 else b + step), rows)]
        way = k % 2
        dst = opp2[i].at[l, way] if k < 2 else fin2[i].at[l, way, rows]
        return remote(src, dst, send2.at[i], (early2 if k < 2 else late2).at[i], device(l, a, b + step))

    def add(i, rows, block, *terms):
        start, height = rows.start, rows.size

        def body(r, c, carry):
            r = pl.ds(pl.multiple_of(r.start + start, ROWS), ROWS)
            total = whole[i][(*block, r, c)].astype(F32)
            for ref, lead, first in terms:
                total = total + ref[(*lead, pl.ds(pl.multiple_of(r.start - first, ROWS), ROWS), c)].astype(F32)
            whole[i][(*block, r, c)] = total.astype(BF16)
            return carry

        tiles(height, size[i][1], body)(0)

    def opposite1(i, j):
        landed(opp1[i].at[:, :, j], early1.at[i, j])

    def final1(i, j):
        landed(fin1[i].at[:, :, j], late1.at[i, j])

    def opposite2(i):
        landed(opp2[i], early2.at[i])

    def final2(i):
        landed(fin2[i], late2.at[i])

    def load(l, i, s):
        a, _ = ab(l)
        slab, rows = lax.rem(a + (1, 3, 0)[s], side), (low, high, everything)[s][i]
        where = (l, slab, slice(None), rows) if l == 0 else (l, slice(None), slab, rows)
        return pltpu.make_async_copy(g[i].at[where], whole[i].at[where], load_sem.at[i, s // 2])

    def states(i):
        return (
            pltpu.make_async_copy(m[i], new_m[i], state_sem.at[i, 0]),
            pltpu.make_async_copy(v[i], new_v[i], state_sem.at[i, 0]),
            *(pltpu.make_async_copy(w[i].at[l, x, y], own_w[i].at[l], state_sem.at[i, 1]) for l in layers),
        )

    def stage(l, s):
        a, b = ab(l)
        off, rows = ((2, everything), (1, high), (3, low))[s]
        where = (*at(l, a + off, b + 2), rows[0])
        return pltpu.make_async_copy(g[0].at[where], whole[0].at[where], stage_sem)

    wait_for_neighbours = torus.greet()
    for l in layers:
        for s in (0, 1, 2):
            stage(l, s).start()
    for i in which:
        for l in layers:
            for s in (0, 1):
                load(l, i, s).start()
    wait_for_neighbours()

    @pl.when(lax.rem(lax.axis_index("rep"), 2) == 0)
    def _():
        pl.delay(LATER)

    def send_raw(i, j, staged=False):
        for k in (0, 1, 2, 3):
            for l in layers:
                sum1(k, l, i, j, staged).start()

    def pass_on1(i, j, first):
        if first:
            landed(whole[i].at[0, :2], load_sem.at[i, 0])
        opposite1(i, j)
        for l in layers:
            a, b = ab(l)
            for k in (0, 1):
                rows = (low, high)[k][i]
                add(i, rows, at(l, a + (1, 3)[k], b + j), (opp1[i], (l, k, j), rows.start))
                sum1(4 + k, l, i, j).start()

    def start2(i):
        landed(whole[i].at[0, :2], load_sem.at[i, 1])
        final1(i, 2)
        for l in layers:
            a, b = ab(l)
            add(i, everything[i], at(l, a, b + 2), (fin1[i], (l, 0, 2), 0), (fin1[i], (l, 1, 2), 0))
            sum2(0, l, i).start()
            sum2(1, l, i).start()
        final1(i, 1)
        final1(i, 3)
        for l in layers:
            a, b = ab(l)
            for k, j, rows in ((2, 1, high), (3, 3, low)):
                add(i, rows[i], at(l, a, b + j), (fin1[i], (l, 0, j), 0), (fin1[i], (l, 1, j), 0))
                sum2(k, l, i).start()

    def pass_on2(i):
        opposite2(i)
        for l in layers:
            a, b = ab(l)
            for k, j, rows in ((0, 1, low), (1, 3, high)):
                add(i, rows[i], at(l, a, b + j), (fin1[i], (l, 0, j), 0), (fin1[i], (l, 1, j), 0), (opp2[i], (l, k), rows[i].start))
                sum2(4 + k, l, i).start()

    def own(i, total):
        final1(i, 0)
        final2(i)
        for l in layers:

            def body(r, c, total, l=l):
                s = whole[i][l, x, y, r, c].astype(F32)
                for ref, lead in ((fin1[i], (l, 0, 0)), (fin1[i], (l, 1, 0)), (fin2[i], (l, 0)), (fin2[i], (l, 1))):
                    s = s + ref[(*lead, r, c)].astype(F32)
                s = s.astype(BF16)
                whole[i][l, x, y, r, c] = s
                s = s.astype(F32)
                return total + s * s

            total = tiles(*size[i], body)(total)
        return total

    def order(t):
        return (3 - t) * (4 - t) // 2 % side

    landed(whole[0].at[0, 0], stage_sem)
    send_raw(0, 2, True)

    for i in which:
        for l in layers:
            load(l, i, 2).start()
        for one in states(i):
            one.start()

    def sums(t, first):
        for i in which:
            send_raw((i + 1) % 3, order(t) if i < 2 else order(t + 1))
            pass_on1(i, order(t), first)

    sums(0, True)

    def more(t, carry):
        sums(t, False)
        return carry

    lax.fori_loop(1, side - 1, more, 0)
    for i in which:
        if i < 2:
            send_raw(i + 1, 0)
        start2(i)
        if i > 0:
            pass_on2(i - 1)
        pass_on1(i, 0, False)
    pass_on2(2)

    total = jnp.zeros((ROWS, COLUMNS), F32)
    for i in which:
        total = own(i, total)
    total = jnp.sum(total.reshape(ROWS // 8, 8, COLUMNS), 0)
    mine[...] = functools.reduce(jnp.add, [total[:, 128 * q : 128 * (q + 1)] for q in range(COLUMNS // 128)])

    gathers = [Gather(torus, whole[i], *(sem.at[i] for sem in (send1, send2, early1, late1, early2, late2))) for i in which]
    for one in gathers:
        one.sent()

    def share(k):
        return remote(mine, squares.at[me], send_sq, recv_sq, {"dp": lax.rem(me + k, n)})

    lax.fori_loop(1, n, lambda k, c: (share(k).start(), c)[1], 0)
    squares[me] = mine[...]
    for i in which:
        landed(whole[i].at[0, :2], state_sem.at[i, 0])
        landed(own_w[i], state_sem.at[i, 1])
    landed(squares.at[: n - 1], recv_sq)
    total = functools.reduce(jnp.add, [squares[k] for k in range(n)])
    total = jnp.full((8, 128), jnp.sum(total), F32)
    factor = jnp.max(jnp.minimum(1.0, 0.5 * lax.rsqrt(total / count + 1e-30)))

    def update(l, i, rows):
        def body(r, c, carry):
            r = pl.ds(pl.multiple_of(r.start + rows.start, ROWS), ROWS)
            grad = whole[i][l, x, y, r, c].astype(F32) * factor
            old = own_w[i][l, r, c].astype(F32)
            moment = 0.9 * new_m[i][l, r, c] + 0.1 * grad
            square = 0.95 * new_v[i][l, r, c] + 0.05 * grad * grad
            step = moment * lax.rsqrt(square + 1e-8) + 0.1 * old
            new = (old - 0.02 * step).astype(BF16)
            if i < 2:
                whole[i][l, x, y, r, c] = new
            else:
                left[l, r, c] = new
            new_m[i][l, r, c] = moment
            new_v[i][l, r, c] = square
            return carry

        tiles(rows.size, size[i][1], body)(0)

    one, two, _ = gathers
    for l in layers:
        for rows, ks in ((low, (0, 3)), (high, (1, 2))):
            update(l, 0, rows[0])
            for k in ks:
                one.copy2(k, l).start()
                one.copy1(k, l, 0).start()
    for l in layers:
        update(l, 1, everything[1])
    two.first2()
    one.forward2()
    two.first1(0)
    for l in layers:
        update(l, 2, everything[2])
    two.forward2()
    one.forward1(0)
    one.final2()
    one.first1(1)
    two.forward1(0)
    two.final2()
    two.first1(1)
    one.forward1(1)

    def rest(t, carry):
        one.first1(back(t, side))
        two.forward1(back(t - 1, side))
        two.first1(back(t, side))
        one.forward1(back(t, side))
        return carry

    lax.fori_loop(2, side, rest, 0)
    two.forward1(back(side - 1, side))
    one.finish()
    two.finish()
    landed(squares.at[: n - 1], send_sq)


def gather_last(n, block, whole, send1, send2, early1, late1, early2, late2, own_sem):
    torus = Torus(n)
    wait_for_neighbours = torus.greet()
    own = pltpu.make_async_copy(block, whole.at[:, torus.x, torus.y], own_sem)
    own.start()
    wait_for_neighbours()
    own.wait()
    one = Gather(torus, whole, send1, send2, early1, late1, early2, late2)
    one.first2()
    one.first1(0)
    one.forward2()
    one.forward1(0)
    one.final2()
    one.first1(1)

    def rest(t, carry):
        one.first1(back(t, torus.side))
        one.forward1(back(t - 1, torus.side))
        return carry

    lax.fori_loop(2, torus.side, rest, 0)
    one.forward1(back(torus.side - 1, torus.side))
    one.finish()


def drain(*refs):
    sources, targets, sem = refs[: len(refs) // 2], refs[len(refs) // 2 : -1], refs[-1]
    copies = [pltpu.make_async_copy(s, t, sem.at[k]) for k, (s, t) in enumerate(zip(sources, targets, strict=True))]
    for copy in copies:
        copy.start()
    for copy in copies:
        copy.wait()


def solution(mesh):
    n = mesh.shape["dp"]
    side = math.isqrt(n)

    def step(*arrays):
        terms, weights, m, v = (arrays[i : i + 3] for i in (0, 3, 6, 9))
        count = n * sum(one.size for one in m)
        blocks = [one.shape for one in m]
        grid = [(l, side, side, r, c) for l, r, c in blocks]
        any_of = pl.BlockSpec(memory_space=pl.ANY)
        half = lambda *lead: [pltpu.VMEM((*lead, r // 2, c), BF16) for _, r, c in blocks]
        full = lambda *lead: [pltpu.VMEM((*lead, r, c), BF16) for _, r, c in blocks]
        dma = pltpu.SemaphoreType.DMA
        in_vmem = pl.BlockSpec(memory_space=pltpu.VMEM)

        def copy_out(arrays, name):
            return pl.pallas_call(
                drain,
                out_shape=[pltpu.HBM(one.shape, one.dtype) for one in arrays],
                in_specs=[any_of] * len(arrays),
                out_specs=[any_of] * len(arrays),
                scratch_shapes=[dma((len(arrays),))],
                compiler_params=pltpu.CompilerParams(vmem_limit_bytes=1 << 20),
                name=name,
            )(*(pltpu.with_memory_space_constraint(one, pltpu.VMEM) for one in arrays))

        out = pl.pallas_call(
            functools.partial(kernel, n, count),
            out_shape=[pltpu.VMEM(one, BF16) for one in grid[:2]] + [pltpu.VMEM(one, F32) for one in blocks] * 2 + [pltpu.VMEM(blocks[2], BF16)],
            in_specs=[any_of] * 12,
            out_specs=[in_vmem] * 9,
            scratch_shapes=[
                pltpu.VMEM(grid[2], BF16),
                *half(2, 2, side),
                *full(2, 2, side),
                *half(2, 2),
                *full(2, 2),
                *full(2),
                pltpu.VMEM((n, 8, 128), F32),
                pltpu.VMEM((8, 128), F32),
                dma((3, 2)),
                dma((3, 2)),
                dma((3,)),
                dma((3,)),
                dma((3, side)),
                dma((3, side)),
                dma((3,)),
                dma((3,)),
                dma,
                dma,
                dma,
            ],
            compiler_params=pltpu.CompilerParams(collective_id=0, has_side_effects=True, vmem_limit_bytes=33 << 20),
            name="step",
        )(
            *(t.reshape(one) for t, one in zip(terms, grid, strict=True)),
            *(t.reshape(one) for t, one in zip(weights, grid, strict=True)),
            *m,
            *v,
        )
        gate, up, *moments, left = copy_out(out, "copy_out")
        (last,) = pl.pallas_call(
            functools.partial(gather_last, n),
            out_shape=[pltpu.VMEM(grid[2], BF16)],
            in_specs=[any_of],
            out_specs=[in_vmem],
            scratch_shapes=[dma, dma, dma((side,)), dma((side,)), dma, dma, dma],
            compiler_params=pltpu.CompilerParams(collective_id=1, has_side_effects=True, vmem_limit_bytes=1 << 20),
            name="gather_last",
        )(pltpu.with_memory_space_constraint(left, pltpu.HBM))
        (down,) = copy_out([last], "copy_last_out")
        return (*(one.reshape(w.shape) for one, w in zip((gate, up, down), weights, strict=True)), *moments)

    all_of, cut = P(None, None, None), P(None, "dp", None)
    return jax.shard_map(
        step,
        mesh=mesh,
        in_specs=(P(("rep", "dp"), None, None, None),) * 3 + (all_of,) * 3 + (cut,) * 6,
        out_specs=(P("rep", None, None),) * 3 + (P("rep", "dp", None),) * 6,
        check_vma=False,
    )
```

```python
import functools
import math

import jax
import jax.numpy as jnp
from jax import lax
from jax.experimental import pallas as pl
from jax.experimental.pallas import tpu as pltpu
from jax.sharding import PartitionSpec as P

MESH = pl.DeviceIdType.MESH
LAYERS = (0, 1)
ROWS, COLUMNS = 16, 512
LATER = 8_200
BF16, F32 = jnp.bfloat16, jnp.float32


def tiles(rows, columns, body):
    across = columns // COLUMNS

    def one(t, carry):
        r, c = t // across, t % across
        return body(pl.ds(pl.multiple_of(r * ROWS, ROWS), ROWS), pl.ds(pl.multiple_of(c * COLUMNS, COLUMNS), COLUMNS), carry)

    return functools.partial(lax.fori_loop, 0, (rows // ROWS) * across, one)


class Torus:
    def __init__(self, n):
        self.side = math.isqrt(n)
        self.me = lax.axis_index("dp")
        self.x, self.y = self.me // self.side, self.me % self.side

    def ab(self, l):
        return (self.x, self.y) if l == 0 else (self.y, self.x)

    def at(self, l, a, b):
        a, b = lax.rem(a, self.side), lax.rem(b, self.side)
        return (l, a, b) if l == 0 else (l, b, a)

    def device(self, l, a, b):
        _, p, q = self.at(l, a, b)
        return {"dp": p * self.side + q}

    def greet(self):
        barrier = pltpu.get_barrier_semaphore()
        for l in LAYERS:
            a, b = self.ab(l)
            for step in (1, 3):
                pl.semaphore_signal(barrier, inc=1, device_id=self.device(l, a + step, b), device_id_type=MESH)
        return lambda: pl.semaphore_wait(barrier, 4)


def remote(src, dst, send, recv, target):
    return pltpu.make_async_remote_copy(src_ref=src, dst_ref=dst, send_sem=send, recv_sem=recv, device_id=target, device_id_type=MESH)


def landed(ref, sem):
    pltpu.make_async_copy(ref, ref, sem).wait()


class Gather:
    def __init__(self, torus, whole, send1, send2, early1, late1, early2, late2):
        self.torus, self.whole = torus, whole
        self.send1, self.send2, self.early1, self.late1, self.early2, self.late2 = send1, send2, early1, late1, early2, late2
        rows = whole.shape[-2]
        low, high = pl.ds(0, rows // 2), pl.ds(rows // 2, rows // 2)
        self.kinds = ((1, low, 0), (3, high, 0), (1, high, 0), (3, low, 0), (1, low, 3), (3, high, 1))

    def copy2(self, k, l):
        a, b = self.torus.ab(l)
        step, rows, off = self.kinds[k]
        block = self.whole.at[(*self.torus.at(l, a, b + off), rows)]
        return remote(block, block, self.send2, self.early2 if k < 2 else self.late2, self.torus.device(l, a, b + step))

    def copy1(self, k, l, j):
        a, b = self.torus.ab(l)
        step, rows, off = self.kinds[k]
        block = self.whole.at[(*self.torus.at(l, a + off, b + j), rows)]
        return remote(block, block, self.send1, (self.early1 if k < 2 else self.late1).at[j], self.torus.device(l, a + step, b))

    def first2(self):
        for k in (0, 1, 2, 3):
            for l in LAYERS:
                self.copy2(k, l).start()

    def forward2(self):
        landed(self.whole.at[0, 0, :2], self.early2)
        for k in (4, 5):
            for l in LAYERS:
                self.copy2(k, l).start()

    def final2(self):
        landed(self.whole.at[0, 0], self.late2)

    def first1(self, j):
        for k in (0, 1, 2, 3):
            for l in LAYERS:
                self.copy1(k, l, j).start()

    def forward1(self, j):
        landed(self.whole.at[0, 0, :2], self.early1.at[j])
        for k in (4, 5):
            for l in LAYERS:
                self.copy1(k, l, j).start()

    def finish(self):
        for j in range(self.torus.side):
            landed(self.whole.at[0, 0], self.late1.at[j])
        self.sent()

    def sent(self):
        landed(self.whole.at[:, :3], self.send1)
        landed(self.whole.at[:, :3, 0], self.send2)


def back(t, side):
    return t * (t + 1) // 2 % side


def kernel(n, count, *refs):
    side = math.isqrt(n)
    g, w, m, v = (refs[3 * i : 3 * i + 3] for i in range(4))
    new_m, new_v = refs[14:17], refs[17:20]
    left = refs[20]
    whole = (*refs[12:14], refs[21])
    opp1, fin1, opp2, fin2, own_w = (refs[22 + 3 * i : 25 + 3 * i] for i in range(5))
    squares, mine, load_sem, state_sem, send1, send2, early1, late1, early2, late2, send_sq, recv_sq, stage_sem = refs[37:]

    torus = Torus(n)
    me, x, y, ab, at, device = torus.me, torus.x, torus.y, torus.ab, torus.at, torus.device
    layers, which = LAYERS, (0, 1, 2)
    size = [(r.shape[-2], r.shape[-1]) for r in new_m]
    low = [pl.ds(0, r // 2) for r, _ in size]
    high = [pl.ds(r // 2, r // 2) for r, _ in size]
    everything = [pl.ds(0, r) for r, _ in size]

    def sum1(k, l, i, j, staged=False):
        a, b = ab(l)
        step, rows = ((1, low), (3, high), (1, high), (3, low), (1, low), (3, high))[k]
        rows = rows[i]
        block = at(l, a + 2 if k < 2 else a + step, b + j)
        src = (whole if staged or k > 3 else g)[i].at[(*block, rows)]
        way = k % 2
        dst = opp1[i].at[l, way, j] if k < 2 else fin1[i].at[l, way, j, rows]
        return remote(src, dst, send1.at[i], (early1 if k < 2 else late1).at[i, j], device(l, a + step, b))

    def sum2(k, l, i):
        a, b = ab(l)
        step, rows = ((1, low), (3, high), (1, high), (3, low), (1, low), (3, high))[k]
        rows = rows[i]
        src = whole[i].at[(*at(l, a, b + 2 if k < 2 else b + step), rows)]
        way = k % 2
        dst = opp2[i].at[l, way] if k < 2 else fin2[i].at[l, way, rows]
        return remote(src, dst, send2.at[i], (early2 if k < 2 else late2).at[i], device(l, a, b + step))

    def add(i, rows, block, *terms):
        start, height = rows.start, rows.size

        def body(r, c, carry):
            r = pl.ds(pl.multiple_of(r.start + start, ROWS), ROWS)
            total = whole[i][(*block, r, c)].astype(F32)
            for ref, lead, first in terms:
                total = total + ref[(*lead, pl.ds(pl.multiple_of(r.start - first, ROWS), ROWS), c)].astype(F32)
            whole[i][(*block, r, c)] = total.astype(BF16)
            return carry

        tiles(height, size[i][1], body)(0)

    def opposite1(i, j):
        landed(opp1[i].at[:, :, j], early1.at[i, j])

    def final1(i, j):
        landed(fin1[i].at[:, :, j], late1.at[i, j])

    def opposite2(i):
        landed(opp2[i], early2.at[i])

    def final2(i):
        landed(fin2[i], late2.at[i])

    def load(l, i, s):
        a, _ = ab(l)
        slab, rows = lax.rem(a + (1, 3, 0)[s], side), (low, high, everything)[s][i]
        where = (l, slab, slice(None), rows) if l == 0 else (l, slice(None), slab, rows)
        return pltpu.make_async_copy(g[i].at[where], whole[i].at[where], load_sem.at[i, s // 2])

    def states(i):
        return (
            pltpu.make_async_copy(m[i], new_m[i], state_sem.at[i, 0]),
            pltpu.make_async_copy(v[i], new_v[i], state_sem.at[i, 0]),
            *(pltpu.make_async_copy(w[i].at[l, x, y], own_w[i].at[l], state_sem.at[i, 1]) for l in layers),
        )

    def stage(l, s):
        a, b = ab(l)
        off, rows = ((2, everything), (1, high), (3, low))[s]
        where = (*at(l, a + off, b + 2), rows[0])
        return pltpu.make_async_copy(g[0].at[where], whole[0].at[where], stage_sem)

    wait_for_neighbours = torus.greet()
    for l in layers:
        for s in (0, 1, 2):
            stage(l, s).start()
    for i in which:
        for l in layers:
            for s in (0, 1):
                load(l, i, s).start()
    wait_for_neighbours()

    @pl.when(lax.rem(lax.axis_index("rep"), 2) == 0)
    def _():
        pl.delay(LATER)

    def send_raw(i, j, staged=False):
        for k in (0, 1, 2, 3):
            for l in layers:
                sum1(k, l, i, j, staged).start()

    def pass_on1(i, j, first):
        if first:
            landed(whole[i].at[0, :2], load_sem.at[i, 0])
        opposite1(i, j)
        for l in layers:
            a, b = ab(l)
            for k in (0, 1):
                rows = (low, high)[k][i]
                add(i, rows, at(l, a + (1, 3)[k], b + j), (opp1[i], (l, k, j), rows.start))
                sum1(4 + k, l, i, j).start()

    def start2(i):
        landed(whole[i].at[0, :2], load_sem.at[i, 1])
        final1(i, 2)
        for l in layers:
            a, b = ab(l)
            add(i, everything[i], at(l, a, b + 2), (fin1[i], (l, 0, 2), 0), (fin1[i], (l, 1, 2), 0))
            sum2(0, l, i).start()
            sum2(1, l, i).start()
        final1(i, 1)
        final1(i, 3)
        for l in layers:
            a, b = ab(l)
            for k, j, rows in ((2, 1, high), (3, 3, low)):
                add(i, rows[i], at(l, a, b + j), (fin1[i], (l, 0, j), 0), (fin1[i], (l, 1, j), 0))
                sum2(k, l, i).start()

    def pass_on2(i):
        opposite2(i)
        for l in layers:
            a, b = ab(l)
            for k, j, rows in ((0, 1, low), (1, 3, high)):
                add(i, rows[i], at(l, a, b + j), (fin1[i], (l, 0, j), 0), (fin1[i], (l, 1, j), 0), (opp2[i], (l, k), rows[i].start))
                sum2(4 + k, l, i).start()

    def own(i, total):
        final1(i, 0)
        final2(i)
        for l in layers:

            def body(r, c, total, l=l):
                s = whole[i][l, x, y, r, c].astype(F32)
                for ref, lead in ((fin1[i], (l, 0, 0)), (fin1[i], (l, 1, 0)), (fin2[i], (l, 0)), (fin2[i], (l, 1))):
                    s = s + ref[(*lead, r, c)].astype(F32)
                s = s.astype(BF16)
                whole[i][l, x, y, r, c] = s
                s = s.astype(F32)
                return total + s * s

            total = tiles(*size[i], body)(total)
        return total

    def order(t):
        return (3 - t) * (4 - t) // 2 % side

    landed(whole[0].at[0, 0], stage_sem)
    send_raw(0, 2, True)

    for i in which:
        for l in layers:
            load(l, i, 2).start()
        for one in states(i):
            one.start()

    def sums(t, first):
        for i in which:
            send_raw((i + 1) % 3, order(t) if i < 2 else order(t + 1))
            pass_on1(i, order(t), first)

    sums(0, True)

    def more(t, carry):
        sums(t, False)
        return carry

    lax.fori_loop(1, side - 1, more, 0)
    for i in which:
        if i < 2:
            send_raw(i + 1, 0)
        start2(i)
        if i > 0:
            pass_on2(i - 1)
        pass_on1(i, 0, False)
    pass_on2(2)

    total = jnp.zeros((ROWS, COLUMNS), F32)
    for i in which:
        total = own(i, total)
    total = jnp.sum(total.reshape(ROWS // 8, 8, COLUMNS), 0)
    mine[...] = functools.reduce(jnp.add, [total[:, 128 * q : 128 * (q + 1)] for q in range(COLUMNS // 128)])

    gathers = [Gather(torus, whole[i], *(sem.at[i] for sem in (send1, send2, early1, late1, early2, late2))) for i in which]
    for one in gathers:
        one.sent()

    def share(k):
        return remote(mine, squares.at[me], send_sq, recv_sq, {"dp": lax.rem(me + k, n)})

    lax.fori_loop(1, n, lambda k, c: (share(k).start(), c)[1], 0)
    squares[me] = mine[...]
    for i in which:
        landed(whole[i].at[0, :2], state_sem.at[i, 0])
        landed(own_w[i], state_sem.at[i, 1])
    landed(squares.at[: n - 1], recv_sq)
    total = functools.reduce(jnp.add, [squares[k] for k in range(n)])
    total = jnp.full((8, 128), jnp.sum(total), F32)
    factor = jnp.max(jnp.minimum(1.0, 0.5 * lax.rsqrt(total / count + 1e-30)))

    def update(l, i, rows):
        def body(r, c, carry):
            r = pl.ds(pl.multiple_of(r.start + rows.start, ROWS), ROWS)
            grad = whole[i][l, x, y, r, c].astype(F32) * factor
            old = own_w[i][l, r, c].astype(F32)
            moment = 0.9 * new_m[i][l, r, c] + 0.1 * grad
            square = 0.95 * new_v[i][l, r, c] + 0.05 * grad * grad
            step = moment * lax.rsqrt(square + 1e-8) + 0.1 * old
            new = (old - 0.02 * step).astype(BF16)
            if i < 2:
                whole[i][l, x, y, r, c] = new
            else:
                left[l, r, c] = new
            new_m[i][l, r, c] = moment
            new_v[i][l, r, c] = square
            return carry

        tiles(rows.size, size[i][1], body)(0)

    one, two, _ = gathers
    for l in layers:
        for rows, ks in ((low, (0, 3)), (high, (1, 2))):
            update(l, 0, rows[0])
            for k in ks:
                one.copy2(k, l).start()
                one.copy1(k, l, 0).start()
    for l in layers:
        update(l, 1, everything[1])
    two.first2()
    one.forward2()
    two.first1(0)
    for l in layers:
        update(l, 2, everything[2])
    two.forward2()
    one.forward1(0)
    one.final2()
    one.first1(1)
    two.forward1(0)
    two.final2()
    two.first1(1)
    one.forward1(1)

    def rest(t, carry):
        one.first1(back(t, side))
        two.forward1(back(t - 1, side))
        two.first1(back(t, side))
        one.forward1(back(t, side))
        return carry

    lax.fori_loop(2, side, rest, 0)
    two.forward1(back(side - 1, side))
    one.finish()
    two.finish()
    landed(squares.at[: n - 1], send_sq)


def gather_last(n, block, whole, send1, send2, early1, late1, early2, late2, own_sem):
    torus = Torus(n)
    wait_for_neighbours = torus.greet()
    own = pltpu.make_async_copy(block, whole.at[:, torus.x, torus.y], own_sem)
    own.start()
    wait_for_neighbours()
    own.wait()
    one = Gather(torus, whole, send1, send2, early1, late1, early2, late2)
    one.first2()
    one.first1(0)
    one.forward2()
    one.forward1(0)
    one.final2()
    one.first1(1)

    def rest(t, carry):
        one.first1(back(t, torus.side))
        one.forward1(back(t - 1, torus.side))
        return carry

    lax.fori_loop(2, torus.side, rest, 0)
    one.forward1(back(torus.side - 1, torus.side))
    one.finish()


def together(sources, targets, sem):
    copies = [pltpu.make_async_copy(p, q, sem.at[k]) for k, (p, q) in enumerate(zip(sources, targets, strict=True))]
    for copy in copies:
        copy.start()
    for copy in copies:
        copy.wait()


def drain(*refs):
    later = lax.rem(lax.axis_index("rep"), 2) == 0
    sources, targets, sem = refs[:9], refs[9:18], refs[18]

    @pl.when(later)
    def _():
        together(sources, targets, sem)

    @pl.when(jnp.logical_not(later))
    def _():
        together((*sources[:2], sources[8]), (*targets[:2], targets[8]), sem)


def drain_last(*refs):
    later = lax.rem(lax.axis_index("rep"), 2) == 0
    sources, targets, sem = refs[:7], refs[13:20], refs[20]

    @pl.when(later)
    def _():
        together(sources[:1], targets[:1], sem)

    @pl.when(jnp.logical_not(later))
    def _():
        together(sources, targets, sem)


def solution(mesh):
    n = mesh.shape["dp"]
    side = math.isqrt(n)

    def step(*arrays):
        terms, weights, m, v = (arrays[i : i + 3] for i in (0, 3, 6, 9))
        count = n * sum(one.size for one in m)
        blocks = [one.shape for one in m]
        grid = [(l, side, side, r, c) for l, r, c in blocks]
        any_of = pl.BlockSpec(memory_space=pl.ANY)
        half = lambda *lead: [pltpu.VMEM((*lead, r // 2, c), BF16) for _, r, c in blocks]
        full = lambda *lead: [pltpu.VMEM((*lead, r, c), BF16) for _, r, c in blocks]
        dma = pltpu.SemaphoreType.DMA
        in_vmem = pl.BlockSpec(memory_space=pltpu.VMEM)

        on_hbm = lambda one: pltpu.HBM(one.shape, one.dtype)
        to_vmem = lambda one: pltpu.with_memory_space_constraint(one, pltpu.VMEM)
        plain = pltpu.CompilerParams(vmem_limit_bytes=1 << 20)

        out = pl.pallas_call(
            functools.partial(kernel, n, count),
            out_shape=[pltpu.VMEM(one, BF16) for one in grid[:2]] + [pltpu.VMEM(one, F32) for one in blocks] * 2 + [pltpu.VMEM(blocks[2], BF16)],
            in_specs=[any_of] * 12,
            out_specs=[in_vmem] * 9,
            scratch_shapes=[
                pltpu.VMEM(grid[2], BF16),
                *half(2, 2, side),
                *full(2, 2, side),
                *half(2, 2),
                *full(2, 2),
                *full(2),
                pltpu.VMEM((n, 8, 128), F32),
                pltpu.VMEM((8, 128), F32),
                dma((3, 2)),
                dma((3, 2)),
                dma((3,)),
                dma((3,)),
                dma((3, side)),
                dma((3, side)),
                dma((3,)),
                dma((3,)),
                dma,
                dma,
                dma,
            ],
            compiler_params=pltpu.CompilerParams(collective_id=0, has_side_effects=True, vmem_limit_bytes=33 << 20),
            name="step",
        )(
            *(t.reshape(one) for t, one in zip(terms, grid, strict=True)),
            *(t.reshape(one) for t, one in zip(weights, grid, strict=True)),
            *m,
            *v,
        )
        gate, up, *moments, left = pl.pallas_call(
            drain,
            out_shape=[on_hbm(one) for one in out],
            in_specs=[any_of] * 9,
            out_specs=[any_of] * 9,
            scratch_shapes=[dma((9,))],
            compiler_params=plain,
            name="copy_out",
        )(*map(to_vmem, out))
        (last,) = pl.pallas_call(
            functools.partial(gather_last, n),
            out_shape=[pltpu.VMEM(grid[2], BF16)],
            in_specs=[any_of],
            out_specs=[in_vmem],
            scratch_shapes=[dma, dma, dma((side,)), dma((side,)), dma, dma, dma],
            compiler_params=pltpu.CompilerParams(collective_id=1, has_side_effects=True, vmem_limit_bytes=1 << 20),
            name="gather_last",
        )(pltpu.with_memory_space_constraint(left, pltpu.HBM))
        down, *moments = pl.pallas_call(
            drain_last,
            out_shape=[on_hbm(one) for one in (last, *moments)],
            in_specs=[any_of] * 13,
            out_specs=[any_of] * 7,
            scratch_shapes=[dma((7,))],
            input_output_aliases={7 + k: 1 + k for k in range(6)},
            compiler_params=plain,
            name="copy_last_out",
        )(*map(to_vmem, (last, *out[2:8])), *moments)
        return (*(one.reshape(w.shape) for one, w in zip((gate, up, down), weights, strict=True)), *moments)

    all_of, cut = P(None, None, None), P(None, "dp", None)
    return jax.shard_map(
        step,
        mesh=mesh,
        in_specs=(P(("rep", "dp"), None, None, None),) * 3 + (all_of,) * 3 + (cut,) * 6,
        out_specs=(P("rep", None, None),) * 3 + (P("rep", "dp", None),) * 6,
        check_vma=False,
    )
```
